256 devices in a mesh: groups: 2 (over y), dp: 32 (over z, core), mp: 4 (over x).
Axes of the slice: x: 4, y: 2, z: 16, core: 2. Of those that a mesh axis runs over, the one named last changes fastest.
The devices are a block of a 4x16x16 slice.
Arguments:
- tokens: bfloat16 [8192, 7168], P(('groups', 'dp')), parts along dimension 0, may hold values from -20 to 20, as said below
- w_down: bfloat16 [7168, 1536], P('dp', 'mp'), may hold values from -3 to 3, as said below
- gain: float32 [1536], P('mp'), may hold values from 0.25 to 1.75
- w_up: bfloat16 [1536, 26112], P('dp', 'mp'), may hold values from -0.15625 to 0.15625
- head_counts: int32 [4], replicated, may hold values from 30 to 34, as said below
- cotangent: bfloat16 [8192, 26112], P(('groups', 'dp'), 'mp'), parts along dimension 0, may hold values from -6 to 6
Outputs:
- queries: bfloat16 [8192, 26112], P(('groups', 'dp'), 'mp'), parts along dimension 0
- grad_tokens: bfloat16 [8192, 7168], P(('groups', 'dp'), 'mp'), parts along dimension 0
The draws below stay inside these ranges and needn't reach their ends.
There are 2 independent parts, one for each index of `groups`. The reference program is written for one: setup_inputs(seed, part) draws one part's arguments, and reference() takes and returns one part's arrays. A program takes and returns all parts, laid end to end along the dimension named above; an argument that names none is the same for every part. Nothing has to cross between parts.
Inputs may be any that keep to these rules, and one draw needn't show every extreme that they name: `tokens`: hidden states of order one with token scales that differ. `w_down`: entries of order 7168^(-1/2). `head_counts`: the entries sum to 128; one of them is 34.
All inputs are finite; a program needn't handle non-finite values.
Results may differ from the reference program's by a relative error of at most 0.018.
Values may be sent and summed in bfloat16 or wider, within the bound.
A program may use at most 128 MiB of HBM per device.

```python
import math
import jax
import jax.numpy as jnp
from jax import lax

D = 7168
LAT = 1536
HEADS = 128
HD = 192
HSLOT = 34
TOKENS = 4096
COLS = 26112
N_MP = 4


def draw_tokens(key, part):
    base_key, scale_key = jax.random.split(key, 2)
    values = jnp.clip(jax.random.normal(base_key, (TOKENS, D), jnp.float32), -6.0, 6.0)
    scales = jnp.exp(jax.random.uniform(scale_key, (TOKENS, 1), jnp.float32, math.log(0.3), math.log(3.0)))
    return (values * scales).astype(jnp.bfloat16)


def draw_w_down(key, part):
    base_key, scale_key = jax.random.split(key, 2)
    values = jax.random.normal(base_key, (D, LAT), jnp.float32)
    values = jnp.clip(values, -6.0, 6.0)
    rising = 0.55 + 1.1 * jnp.arange(LAT, dtype=jnp.float32) / LAT
    col_scale = jnp.exp(jax.random.uniform(scale_key, (1, LAT), jnp.float32, -0.7, 0.7)) * rising
    return (values * col_scale * D ** (-0.5)).astype(jnp.bfloat16)


def draw_head_counts(key, part):
    order_key, extra_key = jax.random.split(jax.random.fold_in(key, 11))
    rank_of = jax.random.permutation(order_key, N_MP).astype(jnp.int32)
    excess = HSLOT - HEADS // N_MP
    extra = jax.random.randint(extra_key, (), 0, excess + 1).astype(jnp.int32)
    delta = jnp.where(rank_of == 0, excess, jnp.where(rank_of == 1, -excess, jnp.where(rank_of == 2, extra, jnp.where(rank_of == 3, -extra, 0))))
    return (HEADS // N_MP + delta).astype(jnp.int32)


def shard_levels(stream_key, extent, shards, smallest, top_value):
    def one(axis_at, blocks):
        steps = jax.random.uniform(jax.random.fold_in(jax.random.fold_in(stream_key, 6), axis_at), (blocks,), jnp.float32, smallest / len(shards), top_value / len(shards))
        return jnp.repeat(jnp.exp(steps), extent[axis_at] // blocks).reshape((-1,) + (1,) * (len(extent) - axis_at - 1))

    level = one(*shards[0])
    for cut in shards[1:]:
        level = level * one(*cut)
    return level


def gaussian(own_key, dims, deviation, most, cuts=(), held_as=jnp.bfloat16):
    array = jax.random.normal(own_key, dims, jnp.float32) * deviation
    if len(cuts) > 0:
        array = shard_levels(own_key, dims, cuts, -0.22, 0.18) * array
    return jnp.clip(array, min=-most, max=most).astype(held_as)


def setup_inputs(seed: int = 0, part: int = 0) -> dict:
    keys = jax.random.split(jax.random.key(seed), 7)
    part_keys = jax.random.split(jax.random.fold_in(keys[6], part), 7)
    return {
        "tokens": draw_tokens(jax.random.fold_in(jax.random.fold_in(keys[6], part), 71), part),
        "w_down": draw_w_down(jax.random.fold_in(keys[6], 71), part),
        "gain": jnp.clip(1.0 + 0.15 * jax.random.normal(keys[2], (LAT,), jnp.float32), 0.25, 1.75),
        "w_up": gaussian(keys[3], (LAT, COLS), LAT ** -0.5, 0.15625, ((0, 32), (1, 4))),
        "head_counts": draw_head_counts(jax.random.fold_in(keys[6], 71), part),
        "cotangent": gaussian(part_keys[5], (TOKENS, COLS), 1.0, 6.0, ((0, 32), (1, 4))),
    }


def reference(tokens, w_down, gain, w_up, head_counts, cotangent):
    latent_raw = jnp.dot(tokens, w_down, preferred_element_type=jnp.float32)
    root_mean = jnp.sqrt(lax.optimization_barrier(jnp.mean(latent_raw * latent_raw, axis=1, keepdims=True)) + 1e-06)
    latent = (latent_raw / root_mean * gain).astype(jnp.bfloat16)
    block_cols = HSLOT * HD
    column = jnp.arange(N_MP * block_cols, dtype=jnp.int32)
    owner = column // block_cols
    slot_index = column % block_cols // HD
    keep_mask = (slot_index < head_counts[owner]).astype(jnp.float32)
    queries = (jnp.dot(latent, w_up, preferred_element_type=jnp.float32) * keep_mask).astype(jnp.bfloat16)
    masked = cotangent * keep_mask.astype(jnp.bfloat16)
    grad_latent = lax.dot_general(masked, w_up, (((1,), (1,)), ((), ())), preferred_element_type=jnp.float32)
    inner_dot = lax.optimization_barrier(jnp.sum(gain * grad_latent * latent_raw, axis=1, keepdims=True))
    grad_raw = (gain * grad_latent / root_mean - latent_raw * inner_dot / (LAT * root_mean ** 3)).astype(jnp.bfloat16)
    width = LAT // N_MP
    running = jnp.zeros((tokens.shape[0], D), jnp.float32)
    for block in range(N_MP):
        product = lax.dot_general(grad_raw[:, block * width:(block + 1) * width], w_down[:, block * width:(block + 1) * width], (((1,), (1,)), ((), ())), preferred_element_type=jnp.float32)
        running = running + lax.optimization_barrier(product.astype(jnp.bfloat16)).astype(jnp.float32)
    return (queries, running.astype(jnp.bfloat16))
```

```python
import functools

import jax
import jax.numpy as jnp
from jax import lax
from jax.experimental import pallas as pl
from jax.experimental.pallas import tpu as pltpu
from jax.sharding import PartitionSpec as P

HD = 192
MESH = pl.DeviceIdType.MESH
F32 = jnp.float32
BF16 = jnp.bfloat16
CHUNK = 384


def kernel(
    tok_h, wd_h, gain_ref, wu_h, heads_ref, cot_h, q_h, gt_h,
    tok, wd, wd2, wu, cot, cot_t, lr_t, lat_t, gain_b, gain_all,
    own_gl, send_gl, peer_gl, grad_raw, q_acc, q_out, gt_out, root,
    load_sem, out_sem, z_send, z_recv, y_send, c_send, c_recv,
    lr_send, lr_recv, ga_send, ga_recv, w2_send, w2_recv, w2c_send, w2c_recv, gl_send, gl_recv,
):
    n_dp, n_mp = lax.axis_size("dp"), lax.axis_size("mp")
    n_z = n_dp // 2
    half = n_z // 2
    me_g, me_dp, me_x = lax.axis_index("groups"), lax.axis_index("dp"), lax.axis_index("mp")
    z, core = me_dp // 2, me_dp % 2
    plane = me_g % 2
    partner = me_g + 1 - 2 * plane
    after, before = (me_dp + 2) % n_dp, (me_dp + n_dp - 2) % n_dp
    sibling = me_dp + 1 - 2 * core

    up_rows, cols = wu_h.shape
    down_rows, lat_cols = wd_h.shape
    n_tok, width = tok_h.shape
    lat = lat_cols * n_mp
    out_cols = width // n_mp
    rows3, cols3 = up_rows // 3, lat_cols // 3
    part_a, part_b, part_c = 2 * plane, 1, 2 * (1 - plane)

    def block(kind, bz, bc):
        if kind == 0:
            return wd.at[pl.ds(pl.multiple_of((2 * bz + bc) * down_rows, down_rows), down_rows), :]
        return wu.at[pl.ds(pl.multiple_of((2 * bz + bc) * up_rows, up_rows), up_rows), :]

    def piece(kind, bz, part):
        if kind == 0:
            rows = pl.ds(pl.multiple_of((2 * bz + core) * down_rows, down_rows), down_rows)
            return wd.at[rows, pl.ds(pl.multiple_of(part * cols3, cols3), cols3)]
        return wu.at[pl.ds(pl.multiple_of((2 * bz + core) * up_rows + part * rows3, rows3), rows3), :]

    def remote(src, dst, send, recv, where):
        return pltpu.make_async_remote_copy(
            src_ref=src, dst_ref=dst, send_sem=send, recv_sem=recv, device_id=where, device_id_type=MESH
        )

    def z_copy(kind, way, bz, part):
        ref = piece(kind, bz, part)
        return remote(
            ref, ref, z_send.at[kind, way, part, bz], z_recv.at[kind, part, bz], {"dp": (after, before)[way]}
        )

    def y_copy(kind, bz, part):
        ref = piece(kind, bz, part)
        return remote(ref, ref, y_send.at[kind, bz], z_recv.at[kind, part, bz], {"groups": partner})

    def c_copy(kind, bz, bc):
        ref = block(kind, bz, bc)
        return remote(ref, ref, c_send.at[kind, bz], c_recv.at[kind, bz], {"dp": sibling})

    def left(s):
        return (z + n_z - s) % n_z

    def right(s):
        return (z + s) % n_z

    own_down = pltpu.make_async_copy(wd_h, block(0, z, core), load_sem.at[0])
    own_up = pltpu.make_async_copy(wu_h, block(1, z, core), load_sem.at[1])
    load_cot = pltpu.make_async_copy(cot_h, cot, load_sem.at[2])
    load_tok = pltpu.make_async_copy(tok_h, tok, load_sem.at[3])
    own_down.start()
    own_up.start()
    load_cot.start()
    load_tok.start()

    barrier = pltpu.get_barrier_semaphore()
    others = [{"dp": after}, {"dp": before}, {"dp": sibling}, {"groups": partner}]
    others += [{"mp": (me_x + i) % n_mp} for i in range(1, n_mp)]
    for where in others:
        pl.semaphore_signal(barrier, inc=1, device_id=where, device_id_type=MESH)
    pl.semaphore_wait(barrier, len(others))

    def send_own(kind):
        for part in (part_a, part_b):
            for way in (0, 1):
                z_copy(kind, way, z, part).start()
        c_copy(kind, z, core).start()

    def ring_step(kind, s):
        lz, rz = left(s), right(s)
        z_copy(kind, 0, lz, part_a).wait_recv()
        z_copy(kind, 0, lz, part_a).start()
        y_copy(kind, lz, part_a).start()
        z_copy(kind, 1, rz, part_a).wait_recv()

        @pl.when(s < half - 1)
        def _():
            z_copy(kind, 1, rz, part_a).start()

        y_copy(kind, rz, part_a).start()
        z_copy(kind, 0, lz, part_b).wait_recv()

        @pl.when(s < half - 1)
        def _():
            z_copy(kind, 0, lz, part_b).start()

        z_copy(kind, 1, rz, part_b).wait_recv()
        z_copy(kind, 1, rz, part_b).start()

    def last_step(kind):
        far = right(half)
        z_copy(kind, 0, far, part_a).wait_recv()
        y_copy(kind, far, part_a).start()
        z_copy(kind, 1, far, part_b).wait_recv()

    def share(kind, bz):
        y_copy(kind, bz, part_c).wait_recv()
        c_copy(kind, bz, core).start()

    def share_pair(kind, s):
        share(kind, left(s))
        share(kind, right(s))

    def wait_sibling(kind, bz):
        c_copy(kind, bz, 1 - core).wait_recv()

    held = jnp.int32(0)
    for i in range(n_mp):
        held = held + jnp.where(me_x == i, heads_ref[i], 0)
    kept = held * HD
    lane = lax.broadcasted_iota(jnp.int32, (1, CHUNK), 1)
    lane1 = lax.broadcasted_iota(jnp.int32, (1, 128), 1)

    own_down.wait()
    send_own(0)
    own_up.wait()
    x_peers = [((me_x + i) % n_mp, (me_x + n_mp - i) % n_mp) for i in range(1, n_mp)]

    def gain_copy(i):
        return remote(
            gain_all.at[me_x], gain_all.at[me_x], ga_send.at[i], ga_recv.at[i], {"mp": x_peers[i][0]}
        )

    gain_all[me_x] = gain_ref[...]
    load_cot.wait()
    n_blocks = cols // 128
    per_step = -(-n_blocks // (half - 1))

    def turn(j, _):
        at = pl.ds(pl.multiple_of(j * 128, 128), 128)
        value = jnp.where(lane1 + j * 128 < kept, cot[:, at], jnp.zeros((), BF16))
        cot_t[at, :] = value.T
        return 0

    def down_step(s, _):
        ring_step(0, s)
        lax.fori_loop((s - 1) * per_step, jnp.minimum(s * per_step, n_blocks), turn, 0)
        return 0

    lax.fori_loop(1, half, down_step, 0)
    send_own(1)
    for i in range(n_mp - 1):
        gain_copy(i).start()
    last_step(0)

    def share_down(s, _):
        share_pair(0, s)
        return 0

    lax.fori_loop(1, half, share_down, 0)
    share(0, right(half))
    load_tok.wait()

    def wait_down(bz, _):
        wait_sibling(0, bz)
        return 0

    lax.fori_loop(0, n_z, wait_down, 0)

    k_size = width // 7

    def latent_part(k, total):
        at = pl.ds(pl.multiple_of(k * k_size, k_size), k_size)
        return total + jnp.dot(tok[:, at], wd[at, :], preferred_element_type=F32)

    latent_raw = lax.fori_loop(0, 7, latent_part, jnp.zeros((n_tok, lat_cols), F32))

    def lat_rows(owner):
        return pl.ds(pl.multiple_of(owner * lat_cols, lat_cols), lat_cols)

    lr_t[lat_rows(me_x), :] = latent_raw.T

    def lr_copy(i, owner):
        ref = lr_t.at[lat_rows(owner), :]
        return remote(ref, ref, lr_send.at[i], lr_recv.at[i], {"mp": x_peers[i][0]})

    half_out = out_cols // 2

    def w2_copy(i):
        to, came_from = x_peers[i]
        rows = pl.ds(pl.multiple_of(to * out_cols + core * half_out, half_out), half_out)
        mine = pl.ds(pl.multiple_of(core * half_out, half_out), half_out)
        return remote(wd.at[rows, :], wd2.at[me_x, mine, :], w2_send.at[i], w2_recv.at[i], {"mp": to})

    def w2_arrived(i, bc):
        rows = pl.ds(pl.multiple_of(bc * half_out, half_out), half_out)
        return wd2.at[x_peers[i][1], rows, :]

    def w2_share(i, bc):
        ref = w2_arrived(i, bc)
        return remote(ref, ref, w2c_send.at[i], w2c_recv.at[i], {"dp": sibling})

    for i in range(n_mp - 1):
        lr_copy(i, me_x).start()
    for i in range(n_mp - 1):
        w2_copy(i).start()
    r_size = out_cols // 7

    def own_part(k, _):
        to = pl.ds(pl.multiple_of(k * r_size, r_size), r_size)
        came = pl.ds(pl.multiple_of(me_x * out_cols + k * r_size, r_size), r_size)
        wd2[me_x, to, :] = wd[came, :]
        return 0

    lax.fori_loop(0, 7, own_part, 0)

    ring_step(1, 1)

    for i in range(n_mp - 1):
        ref = gain_all.at[x_peers[i][1]]
        remote(ref, ref, ga_send.at[i], ga_recv.at[i], {"mp": x_peers[i][0]}).wait_recv()
    for b in range(n_mp):
        gain_b[b * lat_cols : (b + 1) * lat_cols, :] = jnp.broadcast_to(gain_all[b], (n_tok, lat_cols)).T
    for i in range(n_mp - 1):
        lr_copy(i, x_peers[i][1]).wait_recv()
    squares = jnp.zeros((1, n_tok), F32)
    for b in range(n_mp):
        value = lr_t[b * lat_cols : (b + 1) * lat_cols, :]
        squares = squares + jnp.sum(value * value, axis=0, keepdims=True)
    root[...] = jnp.sqrt(squares / lat + 1e-06)
    for b in range(n_mp):
        at = slice(b * lat_cols, (b + 1) * lat_cols)
        lat_t[at, :] = (lr_t[at, :] / root[...] * gain_b[at, :]).astype(BF16)

    z_rows = 2 * up_rows

    def rows_of(bz):
        return pl.ds(pl.multiple_of(bz * z_rows, z_rows), z_rows)

    def gl_copy(i, bz):
        return remote(
            send_gl.at[rows_of(bz), :], peer_gl.at[i, rows_of(bz), :],
            gl_send.at[i, bz], gl_recv.at[i, bz], {"mp": x_peers[i][0]},
        )

    def publish(bz, value):
        own_gl[rows_of(bz), :] = value
        send_gl[rows_of(bz), :] = value.astype(BF16)

    def send_blocks(zs):
        for bz in zs:
            for i in range(n_mp - 1):
                gl_copy(i, bz).start()

    def chunk_at(c):
        return pl.ds(pl.multiple_of(c * CHUNK, CHUNK), CHUNK)

    n_chunks = cols // CHUNK

    def compute(zs, gl=True, q=True, first=False, final=False):
        lefts = [lat_t[rows_of(bz), :].T for bz in zs] if q else None

        def step(c, totals):
            at = chunk_at(c)
            tiles = [wu[rows_of(bz), at] for bz in zs]
            if q:
                value = jnp.dot(lefts[0], tiles[0], preferred_element_type=F32)
                for one, tile in zip(lefts[1:], tiles[1:]):
                    value = value + jnp.dot(one, tile, preferred_element_type=F32)
                if not first:
                    value = value + q_acc[:, at]
                if final:
                    q_out[:, at] = jnp.where(lane + c * CHUNK < kept, value, 0.0).astype(BF16)
                else:
                    q_acc[:, at] = value
            if gl:
                side = cot_t[at, :]
                totals = tuple(
                    total + jnp.dot(tile, side, preferred_element_type=F32) for total, tile in zip(totals, tiles)
                )
            return totals

        start = tuple(jnp.zeros((z_rows, n_tok), F32) for _ in zs) if gl else ()
        totals = lax.fori_loop(0, n_chunks, step, start)
        if gl:
            for bz, total in zip(zs, totals):
                publish(bz, total)
            send_blocks(zs)

    ring_step(1, 2)
    share_pair(1, 1)
    wait_sibling(1, z)
    compute([z], first=True)

    def up_step(s, _):
        ring_step(1, s)
        share_pair(1, s - 1)
        zs = [left(s - 2), right(s - 2)]
        for bz in zs:
            wait_sibling(1, bz)
        compute(zs)
        return 0

    lax.fori_loop(3, half, up_step, 0)
    last_step(1)
    share_pair(1, half - 1)
    zs = [left(half - 2), right(half - 2)]
    for bz in zs:
        wait_sibling(1, bz)
    compute(zs)
    far = right(half)
    share(1, far)
    zs = [left(half - 1), right(half - 1)]
    for bz in zs:
        wait_sibling(1, bz)
    compute(zs)
    for i in range(n_mp - 1):
        ref = w2_arrived(i, core)
        remote(ref, ref, w2_send.at[i], w2_recv.at[i], {"mp": x_peers[i][0]}).wait_recv()
        w2_share(i, core).start()
    wait_sibling(1, far)
    compute([far], q=False)
    compute([far], gl=False, final=True)
    q_store = pltpu.make_async_copy(q_out, q_h, out_sem.at[0])
    q_store.start()

    def wait_gl(bz, _):
        for i in range(n_mp - 1):
            gl_copy(i, bz).wait_recv()
        return 0

    lax.fori_loop(0, n_z, wait_gl, 0)
    inner = jnp.zeros((1, n_tok), F32)
    for b in range(n_mp):
        at = slice(b * lat_cols, (b + 1) * lat_cols)
        total = own_gl[at, :]
        for i in range(n_mp - 1):
            total = total + peer_gl[i, at, :].astype(F32)
        total = total * gain_b[at, :]
        own_gl[at, :] = total
        inner = inner + jnp.sum(total * lr_t[at, :], axis=0, keepdims=True)
    scale = inner / (lat * root[...] * root[...] * root[...])
    for b in range(n_mp):
        at = slice(b * lat_cols, (b + 1) * lat_cols)
        grad_raw[b] = (own_gl[at, :] / root[...] - lr_t[at, :] * scale).T.astype(BF16)
    for i in range(n_mp - 1):
        w2_share(i, 1 - core).wait_recv()

    def out_part(k, _):
        at = pl.ds(pl.multiple_of(k * r_size, r_size), r_size)
        total = jnp.zeros((n_tok, r_size), F32)
        for b in range(n_mp):
            total = total + lax.dot_general(
                grad_raw[b], wd2[b, at, :], (((1,), (1,)), ((), ())), preferred_element_type=F32
            )
        gt_out[:, at] = total.astype(BF16)
        return 0

    lax.fori_loop(0, 7, out_part, 0)
    gt_store = pltpu.make_async_copy(gt_out, gt_h, out_sem.at[1])
    gt_store.start()

    for kind in (0, 1):

        def drain_own(kind):
            for part in (part_a, part_b):
                for way in (0, 1):
                    z_copy(kind, way, z, part).wait_send()
            c_copy(kind, z, core).wait_send()

        def drain(s, _, kind=kind):
            lz, rz = left(s), right(s)
            z_copy(kind, 0, lz, part_a).wait_send()
            z_copy(kind, 1, rz, part_b).wait_send()

            @pl.when(s < half - 1)
            def _():
                z_copy(kind, 1, rz, part_a).wait_send()
                z_copy(kind, 0, lz, part_b).wait_send()

            for bz in (lz, rz):
                y_copy(kind, bz, part_a).wait_send()
                c_copy(kind, bz, core).wait_send()
            return 0

        drain_own(kind)
        lax.fori_loop(1, half, drain, 0)
        y_copy(kind, far, part_a).wait_send()
        c_copy(kind, far, core).wait_send()

    for i in range(n_mp - 1):
        gain_copy(i).wait_send()
        lr_copy(i, me_x).wait_send()
        w2_copy(i).wait_send()
        w2_share(i, core).wait_send()

    def drain_gl(bz, _):
        for i in range(n_mp - 1):
            gl_copy(i, bz).wait_send()
        return 0

    lax.fori_loop(0, n_z, drain_gl, 0)
    q_store.wait()
    gt_store.wait()


def body(tokens, w_down, gain, w_up, head_counts, cotangent):
    n_dp, n_mp = lax.axis_size("dp"), lax.axis_size("mp")
    n_z = n_dp // 2
    n_tok, width = tokens.shape
    up_rows, cols = w_up.shape
    lat_cols = w_down.shape[1]
    lat = lat_cols * n_mp
    out_cols = width // n_mp
    dma = pltpu.SemaphoreType.DMA
    anywhere = pl.BlockSpec(memory_space=pl.ANY)
    peers = n_mp - 1
    return pl.pallas_call(
        kernel,
        out_shape=(
            jax.ShapeDtypeStruct((n_tok, cols), BF16),
            jax.ShapeDtypeStruct((n_tok, out_cols), BF16),
        ),
        in_specs=[
            anywhere,
            anywhere,
            pl.BlockSpec(memory_space=pltpu.VMEM),
            anywhere,
            pl.BlockSpec(memory_space=pltpu.SMEM),
            anywhere,
        ],
        out_specs=(anywhere, anywhere),
        scratch_shapes=[
            pltpu.VMEM((n_tok, width), BF16),
            pltpu.VMEM((width, lat_cols), BF16),
            pltpu.VMEM((n_mp, out_cols, lat_cols), BF16),
            pltpu.VMEM((lat, cols), BF16),
            pltpu.VMEM((n_tok, cols), BF16),
            pltpu.VMEM((cols, n_tok), BF16),
            pltpu.VMEM((lat, n_tok), F32),
            pltpu.VMEM((lat, n_tok), BF16),
            pltpu.VMEM((lat, n_tok), F32),
            pltpu.VMEM((n_mp, 1, lat_cols), F32),
            pltpu.VMEM((lat, n_tok), F32),
            pltpu.VMEM((lat, n_tok), BF16),
            pltpu.VMEM((peers, lat, n_tok), BF16),
            pltpu.VMEM((n_mp, n_tok, lat_cols), BF16),
            pltpu.VMEM((n_tok, cols), F32),
            pltpu.VMEM((n_tok, cols), BF16),
            pltpu.VMEM((n_tok, out_cols), BF16),
            pltpu.VMEM((1, n_tok), F32),
            dma((4,)),
            dma((2,)),
            dma((2, 2, 3, n_z)),
            dma((2, 3, n_z)),
            dma((2, n_z)),
            dma((2, n_z)),
            dma((2, n_z)),
            dma((peers,)),
            dma((peers,)),
            dma((peers,)),
            dma((peers,)),
            dma((peers,)),
            dma((peers,)),
            dma((peers,)),
            dma((peers,)),
            dma((peers, n_z)),
            dma((peers, n_z)),
        ],
        compiler_params=pltpu.CompilerParams(
            collective_id=0, has_side_effects=True, vmem_limit_bytes=60 * 1024 * 1024
        ),
        name="gather_and_project",
    )(tokens, w_down, gain[None, :], w_up, head_counts, cotangent)


def solution(mesh):
    in_specs = (
        P(("groups", "dp"), None),
        P("dp", "mp"),
        P("mp"),
        P("dp", "mp"),
        P(),
        P(("groups", "dp"), "mp"),
    )
    out_specs = (P(("groups", "dp"), "mp"), P(("groups", "dp"), "mp"))
    return jax.shard_map(body, mesh=mesh, in_specs=in_specs, out_specs=out_specs, check_vma=False)
```

```python
import functools

import jax
import jax.numpy as jnp
from jax import lax
from jax.experimental import pallas as pl
from jax.experimental.pallas import tpu as pltpu
from jax.sharding import PartitionSpec as P

HD = 192
MESH = pl.DeviceIdType.MESH
F32 = jnp.float32
BF16 = jnp.bfloat16


def kernel(
    tok_h, wd_h, gain_ref, wu_h, heads_ref, cot_h, q_h, gt_h,
    tok, wd, wd2, wu, cot, cot_t, lr_t, lat_t, gain_b, gain_all,
    own_gl, send_gl, peer_gl, grad_raw, q_acc, q_out, gt_out, root,
    load_sem, out_sem, z_send, z_recv, y_send, c_send, c_recv,
    lr_send, lr_recv, ga_send, ga_recv, w2_send, w2_recv, w2c_send, w2c_recv, gl_send, gl_recv,
    far_send, far_c_send, far_c_recv,
):
    n_dp, n_mp = lax.axis_size("dp"), lax.axis_size("mp")
    n_z = n_dp // 2
    half = n_z // 2
    me_g, me_dp, me_x = lax.axis_index("groups"), lax.axis_index("dp"), lax.axis_index("mp")
    z, core = me_dp // 2, me_dp % 2
    plane = me_g % 2
    partner = me_g + 1 - 2 * plane
    after, before = (me_dp + 2) % n_dp, (me_dp + n_dp - 2) % n_dp
    sibling = me_dp + 1 - 2 * core

    up_rows, cols = wu_h.shape
    down_rows, lat_cols = wd_h.shape
    n_tok, width = tok_h.shape
    lat = lat_cols * n_mp
    out_cols = width // n_mp
    rows3, cols3 = up_rows // 3, lat_cols // 3
    part_a, part_b, part_c = 2 * plane, 1, 2 * (1 - plane)

    def block(kind, bz, bc):
        if kind == 0:
            return wd.at[pl.ds(pl.multiple_of((2 * bz + bc) * down_rows, down_rows), down_rows), :]
        return wu.at[pl.ds(pl.multiple_of((2 * bz + bc) * up_rows, up_rows), up_rows), :]

    def piece(kind, bz, part):
        if kind == 0:
            rows = pl.ds(pl.multiple_of((2 * bz + core) * down_rows, down_rows), down_rows)
            return wd.at[rows, pl.ds(pl.multiple_of(part * cols3, cols3), cols3)]
        return wu.at[pl.ds(pl.multiple_of((2 * bz + core) * up_rows + part * rows3, rows3), rows3), :]

    def remote(src, dst, send, recv, where):
        return pltpu.make_async_remote_copy(
            src_ref=src, dst_ref=dst, send_sem=send, recv_sem=recv, device_id=where, device_id_type=MESH
        )

    def z_copy(kind, way, bz, part):
        ref = piece(kind, bz, part)
        return remote(
            ref, ref, z_send.at[kind, way, part, bz], z_recv.at[kind, part, bz], {"dp": (after, before)[way]}
        )

    def y_copy(kind, bz, part):
        ref = piece(kind, bz, part)
        return remote(ref, ref, y_send.at[kind, bz], z_recv.at[kind, part, bz], {"groups": partner})

    def c_copy(kind, bz, bc):
        ref = block(kind, bz, bc)
        return remote(ref, ref, c_send.at[kind, bz], c_recv.at[kind, bz], {"dp": sibling})

    def left(s):
        return (z + n_z - s) % n_z

    def right(s):
        return (z + s) % n_z

    own_down = pltpu.make_async_copy(wd_h, block(0, z, core), load_sem.at[0])
    own_up = pltpu.make_async_copy(wu_h, block(1, z, core), load_sem.at[1])
    load_cot = pltpu.make_async_copy(cot_h, cot, load_sem.at[2])
    load_tok = pltpu.make_async_copy(tok_h, tok, load_sem.at[3])
    own_down.start()
    own_up.start()
    load_cot.start()
    load_tok.start()

    barrier = pltpu.get_barrier_semaphore()
    others = [{"dp": after}, {"dp": before}, {"dp": sibling}, {"groups": partner}]
    others += [{"mp": (me_x + i) % n_mp} for i in range(1, n_mp)]
    for where in others:
        pl.semaphore_signal(barrier, inc=1, device_id=where, device_id_type=MESH)
    pl.semaphore_wait(barrier, len(others))

    def send_own_down():
        for part in (part_a, part_b):
            for way in (0, 1):
                z_copy(0, way, z, part).start()
        c_copy(0, z, core).start()

    wide = cols // 3

    def send_own_up(j):
        part = jnp.where(j < 3, part_a, part_b)
        rows = pl.ds(pl.multiple_of((2 * z + core) * up_rows + part * rows3, rows3), rows3)
        ref = wu.at[rows, pl.ds(pl.multiple_of((j % 3) * wide, 128), wide)]
        for way in (0, 1):
            remote(
                ref, ref, z_send.at[1, way, part, z], z_recv.at[1, part, z], {"dp": (after, before)[way]}
            ).start()

    def ring_step(kind, s, between=None):
        lz, rz = left(s), right(s)
        z_copy(kind, 0, lz, part_a).wait_recv()
        z_copy(kind, 0, lz, part_a).start()
        y_copy(kind, lz, part_a).start()
        z_copy(kind, 1, rz, part_a).wait_recv()

        @pl.when(s < half - 1)
        def _():
            z_copy(kind, 1, rz, part_a).start()

        y_copy(kind, rz, part_a).start()
        if between is not None:
            between()
        z_copy(kind, 0, lz, part_b).wait_recv()

        @pl.when(s < half - 1)
        def _():
            z_copy(kind, 0, lz, part_b).start()

        z_copy(kind, 1, rz, part_b).wait_recv()
        z_copy(kind, 1, rz, part_b).start()

    far = right(half)

    def share(kind, bz):
        y_copy(kind, bz, part_c).wait_recv()
        c_copy(kind, bz, core).start()

    def share_pair(kind, s):
        share(kind, left(s))
        share(kind, right(s))

    def wait_sibling(kind, bz):
        c_copy(kind, bz, 1 - core).wait_recv()

    n_lane_tiles = cols // 128
    cut = (n_lane_tiles + 1) // 2 * 128

    def far_part(bz):
        return pl.ds(pl.multiple_of((2 * bz + core) * up_rows + part_c * rows3, rows3), rows3)

    def far_copy(way):
        bz = (left, right)[way](half - 1)
        ref = wu.at[far_part(bz), (slice(0, cut), slice(cut, cols))[way]]
        return remote(ref, ref, far_send.at[way], z_recv.at[1, part_c, bz], {"dp": (after, before)[way]})

    def far_share(piece_of, bc):
        base = (2 * far + bc) * up_rows
        if piece_of == 0:
            rows = pl.ds(pl.multiple_of(base + plane * rows3, rows3), 2 * rows3)
        else:
            rows = pl.ds(pl.multiple_of(base + part_c * rows3, rows3), rows3)
        ref = wu.at[rows, :]
        return remote(ref, ref, far_c_send.at[piece_of], far_c_recv.at[piece_of], {"dp": sibling})

    held = jnp.int32(0)
    for i in range(n_mp):
        held = held + jnp.where(me_x == i, heads_ref[i], 0)
    kept = held * HD
    lane1 = lax.broadcasted_iota(jnp.int32, (1, 128), 1)

    own_down.wait()
    send_own_down()
    own_up.wait()
    c_copy(1, z, core).start()
    x_peers = [((me_x + i) % n_mp, (me_x + n_mp - i) % n_mp) for i in range(1, n_mp)]

    def gain_copy(i):
        return remote(
            gain_all.at[me_x], gain_all.at[me_x], ga_send.at[i], ga_recv.at[i], {"mp": x_peers[i][0]}
        )

    gain_all[me_x] = gain_ref[...].reshape(1, lat_cols)
    load_cot.wait()
    n_blocks = cols // 128
    per_step = -(-n_blocks // (half - 1))

    def turn(j, _):
        at = pl.ds(pl.multiple_of(j * 128, 128), 128)
        value = jnp.where(lane1 + j * 128 < kept, cot[:, at], jnp.zeros((), BF16))
        cot_t[at, :] = value.T
        return 0

    def down_step(s, _):
        def between():
            @pl.when(s > 1)
            def _():
                share_pair(0, s - 1)

        ring_step(0, s, between)

        @pl.when(s <= 6)
        def _():
            send_own_up(s - 1)

        lax.fori_loop((s - 1) * per_step, jnp.minimum(s * per_step, n_blocks), turn, 0)
        return 0

    lax.fori_loop(1, half, down_step, 0)
    for i in range(n_mp - 1):
        gain_copy(i).start()
    z_copy(0, 0, far, part_a).wait_recv()
    y_copy(0, far, part_a).start()
    z_copy(0, 1, far, part_b).wait_recv()
    share_pair(0, half - 1)
    ring_step(1, 1)
    share(0, far)
    load_tok.wait()

    def wait_down(bz, _):
        wait_sibling(0, bz)
        return 0

    lax.fori_loop(0, n_z, wait_down, 0)

    k_size = width // 7

    def latent_part(k, total):
        at = pl.ds(pl.multiple_of(k * k_size, k_size), k_size)
        return total + jnp.dot(tok[:, at], wd[at, :], preferred_element_type=F32)

    latent_raw = lax.fori_loop(0, 7, latent_part, jnp.zeros((n_tok, lat_cols), F32))

    def lat_rows(owner):
        return pl.ds(pl.multiple_of(owner * lat_cols, lat_cols), lat_cols)

    lr_t[lat_rows(me_x), :] = latent_raw.T

    def lr_copy(i, owner):
        ref = lr_t.at[lat_rows(owner), :]
        return remote(ref, ref, lr_send.at[i], lr_recv.at[i], {"mp": x_peers[i][0]})

    half_out = out_cols // 2

    def w2_copy(i):
        to, came_from = x_peers[i]
        rows = pl.ds(pl.multiple_of(to * out_cols + core * half_out, half_out), half_out)
        mine = pl.ds(pl.multiple_of(core * half_out, half_out), half_out)
        return remote(wd.at[rows, :], wd2.at[me_x, mine, :], w2_send.at[i], w2_recv.at[i], {"mp": to})

    def w2_arrived(i, bc):
        rows = pl.ds(pl.multiple_of(bc * half_out, half_out), half_out)
        return wd2.at[x_peers[i][1], rows, :]

    def w2_share(i, bc):
        ref = w2_arrived(i, bc)
        return remote(ref, ref, w2c_send.at[i], w2c_recv.at[i], {"dp": sibling})

    for i in range(n_mp - 1):
        lr_copy(i, me_x).start()
    for i in range(n_mp - 1):
        w2_copy(i).start()
    r_size = out_cols // 7

    def own_part(k, _):
        to = pl.ds(pl.multiple_of(k * r_size, r_size), r_size)
        came = pl.ds(pl.multiple_of(me_x * out_cols + k * r_size, r_size), r_size)
        wd2[me_x, to, :] = wd[came, :]
        return 0

    lax.fori_loop(0, 7, own_part, 0)

    ring_step(1, 2, lambda: share_pair(1, 1))
    ring_step(1, 3, lambda: share_pair(1, 2))

    for i in range(n_mp - 1):
        ref = gain_all.at[x_peers[i][1]]
        remote(ref, ref, ga_send.at[i], ga_recv.at[i], {"mp": x_peers[i][0]}).wait_recv()
    for b in range(n_mp):
        gain_b[b * lat_cols : (b + 1) * lat_cols, :] = jnp.broadcast_to(gain_all[b], (n_tok, lat_cols)).T
    for i in range(n_mp - 1):
        lr_copy(i, x_peers[i][1]).wait_recv()
    squares = jnp.zeros((1, n_tok), F32)
    for b in range(n_mp):
        value = lr_t[b * lat_cols : (b + 1) * lat_cols, :]
        squares = squares + jnp.sum(value * value, axis=0, keepdims=True)
    root[...] = jnp.sqrt(squares / lat + 1e-06)
    for b in range(n_mp):
        at = slice(b * lat_cols, (b + 1) * lat_cols)
        lat_t[at, :] = (lr_t[at, :] / root[...] * gain_b[at, :]).astype(BF16)

    z_rows = 2 * up_rows

    def rows_of(bz):
        return pl.ds(pl.multiple_of(bz * z_rows, z_rows), z_rows)

    def gl_copy(i, bz):
        return remote(
            send_gl.at[rows_of(bz), :], peer_gl.at[i, rows_of(bz), :],
            gl_send.at[i, bz], gl_recv.at[i, bz], {"mp": x_peers[i][0]},
        )

    def publish(bz, value):
        own_gl[rows_of(bz), :] = value
        send_gl[rows_of(bz), :] = value.astype(BF16)

    def send_blocks(zs):
        for bz in zs:
            for i in range(n_mp - 1):
                gl_copy(i, bz).start()

    tiles = [(off, min(256, wide - off)) for off in range(0, wide, 256)]

    def compute(zs, gl=True, q=True, first=False, final=False):
        if q:
            one = jnp.concatenate([lat_t[rows_of(bz), :] for bz in zs], axis=0).T

        def step(c, total):
            for off, size in tiles:
                at = pl.ds(pl.multiple_of(c * wide + off, 128), size)
                tile = jnp.concatenate([wu[rows_of(bz), at] for bz in zs], axis=0)
                if gl:
                    total = total + jnp.dot(tile, cot_t[at, :], preferred_element_type=F32)
                if q:
                    value = jnp.dot(one, tile, preferred_element_type=F32)
                    if not first:
                        value = value + q_acc[:, at]
                    if final:
                        lane = lax.broadcasted_iota(jnp.int32, (1, size), 1) + (c * wide + off)
                        q_out[:, at] = jnp.where(lane < kept, value, 0.0).astype(BF16)
                    else:
                        q_acc[:, at] = value
            return total

        start = jnp.zeros((z_rows * len(zs), n_tok), F32) if gl else 0
        total = lax.fori_loop(0, 3, step, start)
        if gl:
            for k, bz in enumerate(zs):
                publish(bz, total[k * z_rows : (k + 1) * z_rows])
            send_blocks(zs)

    def compute_pair(s):
        zs = [left(s), right(s)]
        for bz in zs:
            wait_sibling(1, bz)
        compute(zs)

    wait_sibling(1, z)
    compute([z], first=True)
    compute_pair(1)
    ring_step(1, 4, lambda: share_pair(1, 3))

    def catch_up(s, _):
        compute_pair(s)
        return 0

    lax.fori_loop(2, 4, catch_up, 0)

    def up_step(s, _):
        ring_step(1, s, lambda: share_pair(1, s - 1))
        compute_pair(s - 1)
        return 0

    lax.fori_loop(5, half, up_step, 0)
    for i in range(n_mp - 1):
        ref = w2_arrived(i, core)
        remote(ref, ref, w2_send.at[i], w2_recv.at[i], {"mp": x_peers[i][0]}).wait_recv()
        w2_share(i, core).start()
    for way in (0, 1):
        bz = (left, right)[way](half - 1)
        y_copy(1, bz, part_c).wait_recv()
        far_copy(way).start()
        c_copy(1, bz, core).start()
    z_copy(1, 0, far, part_a).wait_recv()
    z_copy(1, 1, far, part_b).wait_recv()
    far_share(0, core).start()
    compute_pair(half - 1)
    z_copy(1, 0, far, part_c).wait_recv()
    far_share(1, core).start()
    far_share(0, 1 - core).wait_recv()
    far_share(1, 1 - core).wait_recv()
    compute([far], q=False)
    compute([far], gl=False, final=True)
    q_store = pltpu.make_async_copy(q_out, q_h, out_sem.at[0])
    q_store.start()

    for kind in (0, 1):
        for part in (part_a, part_b):
            for way in (0, 1):
                z_copy(kind, way, z, part).wait_send()
        c_copy(kind, z, core).wait_send()

        def drain(s, _, kind=kind):
            lz, rz = left(s), right(s)
            z_copy(kind, 0, lz, part_a).wait_send()
            z_copy(kind, 1, rz, part_b).wait_send()

            @pl.when(s < half - 1)
            def _():
                z_copy(kind, 1, rz, part_a).wait_send()
                z_copy(kind, 0, lz, part_b).wait_send()

            for bz in (lz, rz):
                y_copy(kind, bz, part_a).wait_send()
                c_copy(kind, bz, core).wait_send()
            return 0

        lax.fori_loop(1, half, drain, 0)
    y_copy(0, far, part_a).wait_send()
    c_copy(0, far, core).wait_send()
    for i in range(2):
        far_copy(i).wait_send()
        far_share(i, core).wait_send()
    for i in range(n_mp - 1):
        gain_copy(i).wait_send()
        lr_copy(i, me_x).wait_send()
        w2_copy(i).wait_send()
        w2_share(i, core).wait_send()

    def wait_gl(bz, _):
        for i in range(n_mp - 1):
            gl_copy(i, bz).wait_send()
            gl_copy(i, bz).wait_recv()
        return 0

    lax.fori_loop(0, n_z, wait_gl, 0)
    inner = jnp.zeros((1, n_tok), F32)
    for b in range(n_mp):
        at = slice(b * lat_cols, (b + 1) * lat_cols)
        total = own_gl[at, :]
        for i in range(n_mp - 1):
            total = total + peer_gl[i, at, :].astype(F32)
        total = total * gain_b[at, :]
        own_gl[at, :] = total
        inner = inner + jnp.sum(total * lr_t[at, :], axis=0, keepdims=True)
    scale = inner / (lat * root[...] * root[...] * root[...])
    for b in range(n_mp):
        at = slice(b * lat_cols, (b + 1) * lat_cols)
        grad_raw[b] = (own_gl[at, :] / root[...] - lr_t[at, :] * scale).T.astype(BF16)
    for i in range(n_mp - 1):
        w2_share(i, 1 - core).wait_recv()

    for k in range(7):
        at = slice(k * r_size, (k + 1) * r_size)
        total = jnp.zeros((n_tok, r_size), F32)
        for b in range(n_mp):
            total = total + lax.dot_general(
                grad_raw[b], wd2[b, at, :], (((1,), (1,)), ((), ())), preferred_element_type=F32
            )
        gt_out[:, at] = total.astype(BF16)
    gt_store = pltpu.make_async_copy(gt_out, gt_h, out_sem.at[1])
    gt_store.start()

    q_store.wait()
    gt_store.wait()


def write_kernel(q_in, gt_in, q_h, gt_h, q_hold, gt_hold, in_sem, out_sem):
    n_tok = q_in.shape[0]
    quarter = n_tok // 4
    pairs = [(q_in, q_hold, q_h, slice(k * quarter, (k + 1) * quarter)) for k in range(4)]
    pairs.append((gt_in, gt_hold, gt_h, slice(0, n_tok)))

    def load(k):
        src, hold, _, at = pairs[k]
        return pltpu.make_async_copy(src.at[at, :], hold.at[at, :], in_sem.at[k])

    def store(k):
        _, hold, dst, at = pairs[k]
        return pltpu.make_async_copy(hold.at[at, :], dst.at[at, :], out_sem.at[k])

    for k in range(len(pairs)):
        load(k).start()
    for k in range(len(pairs)):
        load(k).wait()
        store(k).start()
    for k in range(len(pairs)):
        store(k).wait()


def body(tokens, w_down, gain, w_up, head_counts, cotangent):
    n_dp, n_mp = lax.axis_size("dp"), lax.axis_size("mp")
    n_z = n_dp // 2
    n_tok, width = tokens.shape
    up_rows, cols = w_up.shape
    lat_cols = w_down.shape[1]
    lat = lat_cols * n_mp
    out_cols = width // n_mp
    dma = pltpu.SemaphoreType.DMA
    anywhere = pl.BlockSpec(memory_space=pl.ANY)
    peers = n_mp - 1
    queries, grad_tokens = pl.pallas_call(
        kernel,
        out_shape=(
            jax.ShapeDtypeStruct((n_tok, cols), BF16),
            jax.ShapeDtypeStruct((n_tok, out_cols), BF16),
        ),
        in_specs=[
            anywhere,
            anywhere,
            pl.BlockSpec(memory_space=pltpu.VMEM),
            anywhere,
            pl.BlockSpec(memory_space=pltpu.SMEM),
            anywhere,
        ],
        out_specs=(anywhere, anywhere),
        scratch_shapes=[
            pltpu.VMEM((n_tok, width), BF16),
            pltpu.VMEM((width, lat_cols), BF16),
            pltpu.VMEM((n_mp, out_cols, lat_cols), BF16),
            pltpu.VMEM((lat, cols), BF16),
            pltpu.VMEM((n_tok, cols), BF16),
            pltpu.VMEM((cols, n_tok), BF16),
            pltpu.VMEM((lat, n_tok), F32),
            pltpu.VMEM((lat, n_tok), BF16),
            pltpu.VMEM((lat, n_tok), F32),
            pltpu.VMEM((n_mp, 1, lat_cols), F32),
            pltpu.VMEM((lat, n_tok), F32),
            pltpu.VMEM((lat, n_tok), BF16),
            pltpu.VMEM((peers, lat, n_tok), BF16),
            pltpu.VMEM((n_mp, n_tok, lat_cols), BF16),
            pltpu.VMEM((n_tok, cols), F32),
            pltpu.VMEM((n_tok, cols), BF16),
            pltpu.VMEM((n_tok, out_cols), BF16),
            pltpu.VMEM((1, n_tok), F32),
            dma((4,)),
            dma((2,)),
            dma((2, 2, 3, n_z)),
            dma((2, 3, n_z)),
            dma((2, n_z)),
            dma((2, n_z)),
            dma((2, n_z)),
            dma((peers,)),
            dma((peers,)),
            dma((peers,)),
            dma((peers,)),
            dma((peers,)),
            dma((peers,)),
            dma((peers,)),
            dma((peers,)),
            dma((peers, n_z)),
            dma((peers, n_z)),
            dma((2,)),
            dma((2,)),
            dma((2,)),
        ],
        compiler_params=pltpu.CompilerParams(
            collective_id=0, has_side_effects=True, vmem_limit_bytes=60 * 1024 * 1024
        ),
        name="gather_and_project",
    )(tokens, w_down, gain, w_up, head_counts, cotangent)
    return pl.pallas_call(
        write_kernel,
        out_shape=(
            jax.ShapeDtypeStruct((n_tok, cols), BF16),
            jax.ShapeDtypeStruct((n_tok, out_cols), BF16),
        ),
        in_specs=[anywhere, anywhere],
        out_specs=(anywhere, anywhere),
        scratch_shapes=[
            pltpu.VMEM((n_tok, cols), BF16),
            pltpu.VMEM((n_tok, out_cols), BF16),
            dma((5,)),
            dma((5,)),
        ],
        name="write_outputs",
    )(queries, grad_tokens)


def solution(mesh):
    in_specs = (
        P(("groups", "dp"), None),
        P("dp", "mp"),
        P("mp"),
        P("dp", "mp"),
        P(),
        P(("groups", "dp"), "mp"),
    )
    out_specs = (P(("groups", "dp"), "mp"), P(("groups", "dp"), "mp"))
    return jax.shard_map(body, mesh=mesh, in_specs=in_specs, out_specs=out_specs, check_vma=False)
```

```python
import functools

import jax
import jax.numpy as jnp
from jax import lax
from jax.experimental import pallas as pl
from jax.experimental.pallas import tpu as pltpu
from jax.sharding import PartitionSpec as P

HD = 192
MESH = pl.DeviceIdType.MESH
F32 = jnp.float32
BF16 = jnp.bfloat16


def kernel(
    tok_h, wd_h, gain_h, wu_h, heads_h, cot_h, q_h, gt_h,
    tok, wd, wd2, wu, cot, cot_t, lr_t, lat_t, gain_b, gain_all,
    own_gl, send_gl, peer_gl, grad_raw, q_acc, q_out, gt_out, root,
    load_sem, out_sem, z_send, z_recv, y_send, c_send, c_recv,
    lr_send, lr_recv, ga_send, ga_recv, w2_send, w2_recv, w2c_send, w2c_recv, gl_send, gl_recv,
    far_send, far_c_send, far_c_recv, gain_ref, heads_ref,
):
    n_dp, n_mp = lax.axis_size("dp"), lax.axis_size("mp")
    n_z = n_dp // 2
    half = n_z // 2
    me_g, me_dp, me_x = lax.axis_index("groups"), lax.axis_index("dp"), lax.axis_index("mp")
    z, core = me_dp // 2, me_dp % 2
    plane = me_g % 2
    partner = me_g + 1 - 2 * plane
    after, before = (me_dp + 2) % n_dp, (me_dp + n_dp - 2) % n_dp
    sibling = me_dp + 1 - 2 * core

    up_rows, cols = wu_h.shape
    down_rows, lat_cols = wd_h.shape
    n_tok, width = tok_h.shape
    lat = lat_cols * n_mp
    out_cols = width // n_mp
    rows3, cols3 = up_rows // 3, lat_cols // 3
    part_a, part_b, part_c = 2 * plane, 1, 2 * (1 - plane)

    def block(kind, bz, bc):
        if kind == 0:
            return wd.at[pl.ds(pl.multiple_of((2 * bz + bc) * down_rows, down_rows), down_rows), :]
        return wu.at[pl.ds(pl.multiple_of((2 * bz + bc) * up_rows, up_rows), up_rows), :]

    def piece(kind, bz, part):
        if kind == 0:
            rows = pl.ds(pl.multiple_of((2 * bz + core) * down_rows, down_rows), down_rows)
            return wd.at[rows, pl.ds(pl.multiple_of(part * cols3, cols3), cols3)]
        return wu.at[pl.ds(pl.multiple_of((2 * bz + core) * up_rows + part * rows3, rows3), rows3), :]

    def remote(src, dst, send, recv, where):
        return pltpu.make_async_remote_copy(
            src_ref=src, dst_ref=dst, send_sem=send, recv_sem=recv, device_id=where, device_id_type=MESH
        )

    def z_copy(kind, way, bz, part):
        ref = piece(kind, bz, part)
        return remote(
            ref, ref, z_send.at[kind, way, part, bz], z_recv.at[kind, part, bz], {"dp": (after, before)[way]}
        )

    def y_copy(kind, bz, part):
        ref = piece(kind, bz, part)
        return remote(ref, ref, y_send.at[kind, bz], z_recv.at[kind, part, bz], {"groups": partner})

    def c_copy(kind, bz, bc):
        ref = block(kind, bz, bc)
        return remote(ref, ref, c_send.at[kind, bz], c_recv.at[kind, bz], {"dp": sibling})

    def left(s):
        return (z + n_z - s) % n_z

    def right(s):
        return (z + s) % n_z

    own_down = pltpu.make_async_copy(wd_h, block(0, z, core), load_sem.at[0])
    own_up = pltpu.make_async_copy(wu_h, block(1, z, core), load_sem.at[1])
    load_cot = pltpu.make_async_copy(cot_h, cot, load_sem.at[2])
    load_tok = pltpu.make_async_copy(tok_h, tok, load_sem.at[3])
    own_down.start()
    own_up.start()
    load_gain = pltpu.make_async_copy(gain_h, gain_ref, load_sem.at[4])
    load_heads = pltpu.make_async_copy(heads_h, heads_ref, load_sem.at[5])
    load_gain.start()
    load_heads.start()
    load_cot.start()
    load_tok.start()

    barrier = pltpu.get_barrier_semaphore()
    others = [{"dp": after}, {"dp": before}, {"dp": sibling}, {"groups": partner}]
    others += [{"mp": (me_x + i) % n_mp} for i in range(1, n_mp)]
    for where in others:
        pl.semaphore_signal(barrier, inc=1, device_id=where, device_id_type=MESH)
    pl.semaphore_wait(barrier, len(others))

    def send_own_down():
        for part in (part_a, part_b):
            for way in (0, 1):
                z_copy(0, way, z, part).start()
        c_copy(0, z, core).start()

    wide = cols // 3

    def send_own_up(j):
        part = jnp.where(j < 3, part_a, part_b)
        rows = pl.ds(pl.multiple_of((2 * z + core) * up_rows + part * rows3, rows3), rows3)
        ref = wu.at[rows, pl.ds(pl.multiple_of((j % 3) * wide, 128), wide)]
        for way in (0, 1):
            remote(
                ref, ref, z_send.at[1, way, part, z], z_recv.at[1, part, z], {"dp": (after, before)[way]}
            ).start()

    def ring_a(kind, s):
        lz, rz = left(s), right(s)
        z_copy(kind, 0, lz, part_a).wait_recv()
        z_copy(kind, 0, lz, part_a).start()
        y_copy(kind, lz, part_a).start()
        z_copy(kind, 1, rz, part_a).wait_recv()

        @pl.when(s < half - 1)
        def _():
            z_copy(kind, 1, rz, part_a).start()

        y_copy(kind, rz, part_a).start()

    def ring_b(kind, s):
        lz, rz = left(s), right(s)
        z_copy(kind, 0, lz, part_b).wait_recv()

        @pl.when(s < half - 1)
        def _():
            z_copy(kind, 0, lz, part_b).start()

        z_copy(kind, 1, rz, part_b).wait_recv()
        z_copy(kind, 1, rz, part_b).start()

    def ring_step(kind, s, between):
        ring_a(kind, s)
        between()
        ring_b(kind, s)

    far = right(half)

    x_peers = [((me_x + i) % n_mp, (me_x + n_mp - i) % n_mp) for i in range(1, n_mp)]
    per_x = n_z // n_mp

    def w2_at(owner, j, bc):
        return wd2.at[owner, pl.ds(pl.multiple_of((2 * j + bc) * down_rows, down_rows), down_rows), :]

    def w2_copy(bz):
        to = bz // per_x
        j = bz - to * per_x
        slot = (to + n_mp - 1 - me_x) % n_mp
        return remote(block(0, bz, core), w2_at(me_x, j, core), w2_send.at[bz], w2_recv.at[slot, j], {"mp": to})

    def pass_on(bz):
        @pl.when(bz // per_x != me_x)
        def _():
            w2_copy(bz).start()

    def w2_rows(i, j, bc):
        return w2_at(x_peers[i][1], j, bc)

    def w2_share(i, j, bc):
        ref = w2_rows(i, j, bc)
        return remote(ref, ref, w2c_send.at[i, j], w2c_recv.at[i, j], {"dp": sibling})

    def share(kind, bz):
        y_copy(kind, bz, part_c).wait_recv()
        c_copy(kind, bz, core).start()
        if kind == 0:
            pass_on(bz)

    def share_pair(kind, s):
        share(kind, left(s))
        share(kind, right(s))

    def wait_sibling(kind, bz):
        c_copy(kind, bz, 1 - core).wait_recv()

    n_lane_tiles = cols // 128
    cut = n_lane_tiles * 2 // 3 * 128

    def far_part(bz):
        return pl.ds(pl.multiple_of((2 * bz + core) * up_rows + part_c * rows3, rows3), rows3)

    def far_copy(way):
        bz = (left, right)[way](half - 1)
        ref = wu.at[far_part(bz), (slice(0, cut), slice(cut, cols))[way]]
        return remote(ref, ref, far_send.at[way], z_recv.at[1, part_c, bz], {"dp": (after, before)[way]})

    def far_share(piece_of, bc):
        base = (2 * far + bc) * up_rows
        if piece_of == 0:
            rows = pl.ds(pl.multiple_of(base + plane * rows3, rows3), 2 * rows3)
        else:
            rows = pl.ds(pl.multiple_of(base + part_c * rows3, rows3), rows3)
        ref = wu.at[rows, :]
        return remote(ref, ref, far_c_send.at[piece_of], far_c_recv.at[piece_of], {"dp": sibling})

    lane1 = lax.broadcasted_iota(jnp.int32, (1, 128), 1)

    own_down.wait()
    send_own_down()
    own_up.wait()
    send_own_up(0)
    pass_on(z)
    c_copy(1, z, core).start()
    def gain_copy(i):
        return remote(
            gain_all.at[me_x], gain_all.at[me_x], ga_send.at[i], ga_recv.at[i], {"mp": x_peers[i][0]}
        )

    load_gain.wait()
    load_heads.wait()
    held = jnp.int32(0)
    for i in range(n_mp):
        held = held + jnp.where(me_x == i, heads_ref[i], 0)
    kept = held * HD
    gain_all[me_x] = gain_ref[...].reshape(1, lat_cols)
    load_cot.wait()
    n_blocks = cols // 128
    per_step = -(-n_blocks // (half - 1))

    def turn(j, _):
        at = pl.ds(pl.multiple_of(j * 128, 128), 128)
        value = jnp.where(lane1 + j * 128 < kept, cot[:, at], jnp.zeros((), BF16))
        cot_t[at, :] = value.T
        return 0

    def down_step(s, _):
        def between():
            @pl.when(s > 2)
            def _():
                share_pair(0, s - 2)

        ring_step(0, s, between)

        @pl.when(s <= 5)
        def _():
            send_own_up(s)

        @pl.when(s == 4)
        def _():
            z_copy(1, 0, left(1), part_a).wait_recv()
            y_copy(1, left(1), part_a).start()

        @pl.when(s == 5)
        def _():
            z_copy(1, 1, right(1), part_a).wait_recv()
            y_copy(1, right(1), part_a).start()

        @pl.when(s == 6)
        def _():
            z_copy(1, 0, left(1), part_a).start()
            z_copy(1, 1, right(1), part_a).start()

        lax.fori_loop((s - 1) * per_step, jnp.minimum(s * per_step, n_blocks), turn, 0)
        return 0

    lax.fori_loop(1, half, down_step, 0)
    z_copy(1, 0, left(1), part_b).wait_recv()
    z_copy(1, 0, left(1), part_b).start()
    z_copy(1, 1, right(1), part_b).wait_recv()
    z_copy(1, 1, right(1), part_b).start()
    for i in range(n_mp - 1):
        gain_copy(i).start()
    z_copy(0, 0, far, part_a).wait_recv()
    y_copy(0, far, part_a).start()
    z_copy(0, 1, far, part_b).wait_recv()
    ring_a(1, 2)
    share_pair(0, half - 2)
    share_pair(0, half - 1)
    share(0, far)
    ring_b(1, 2)
    load_tok.wait()

    def wait_down(bz, _):
        wait_sibling(0, bz)
        return 0

    lax.fori_loop(0, n_z, wait_down, 0)

    k_size = width // 7

    def latent_part(k, total):
        at = pl.ds(pl.multiple_of(k * k_size, k_size), k_size)
        return total + jnp.dot(tok[:, at], wd[at, :], preferred_element_type=F32)

    latent_raw = lax.fori_loop(0, 7, latent_part, jnp.zeros((n_tok, lat_cols), F32))

    def lat_rows(owner):
        return pl.ds(pl.multiple_of(owner * lat_cols, lat_cols), lat_cols)

    lr_t[lat_rows(me_x), :] = latent_raw.T

    def lr_copy(i, owner):
        ref = lr_t.at[lat_rows(owner), :]
        return remote(ref, ref, lr_send.at[i], lr_recv.at[i], {"mp": x_peers[i][0]})

    for i in range(n_mp - 1):
        lr_copy(i, me_x).start()
    z_rows = 2 * up_rows

    def rows_of(bz):
        return pl.ds(pl.multiple_of(bz * z_rows, z_rows), z_rows)

    def gl_copy(i, bz):
        return remote(
            send_gl.at[rows_of(bz), :], peer_gl.at[i, rows_of(bz), :],
            gl_send.at[i, bz], gl_recv.at[i, bz], {"mp": x_peers[i][0]},
        )

    def publish(bz, value):
        own_gl[rows_of(bz), :] = value
        send_gl[rows_of(bz), :] = value.astype(BF16)

    def send_blocks(zs):
        for bz in zs:
            for i in range(n_mp - 1):
                gl_copy(i, bz).start()

    tiles = [(off, min(256, wide - off)) for off in range(0, wide, 256)]

    def compute(zs, gl=True, q=True, first=False, final=False):
        if q:
            one = jnp.concatenate([lat_t[rows_of(bz), :] for bz in zs], axis=0).T

        def step(c, total):
            for off, size in tiles:
                at = pl.ds(pl.multiple_of(c * wide + off, 128), size)
                tile = jnp.concatenate([wu[rows_of(bz), at] for bz in zs], axis=0)
                if gl:
                    total = total + jnp.dot(tile, cot_t[at, :], preferred_element_type=F32)
                if q:
                    value = jnp.dot(one, tile, preferred_element_type=F32)
                    if not first:
                        value = value + q_acc[:, at]
                    if final:
                        lane = lax.broadcasted_iota(jnp.int32, (1, size), 1) + (c * wide + off)
                        q_out[:, at] = jnp.where(lane < kept, value, 0.0).astype(BF16)
                    else:
                        q_acc[:, at] = value
            return total

        start = jnp.zeros((z_rows * len(zs), n_tok), F32) if gl else 0
        total = lax.fori_loop(0, 3, step, start)
        if gl:
            for k, bz in enumerate(zs):
                publish(bz, total[k * z_rows : (k + 1) * z_rows])
            send_blocks(zs)

    def pair(s):
        return [left(s), right(s)]

    def gl_pair(s):
        for bz in pair(s):
            wait_sibling(1, bz)
        compute(pair(s), q=False)

    def q_pair(s):
        compute(pair(s), gl=False)

    ring_a(1, 3)
    share_pair(1, 1)
    share_pair(1, 2)
    wait_sibling(1, z)
    compute([z], q=False)
    ring_b(1, 3)
    gl_pair(1)
    r_size = out_cols // 7

    def own_part(k, _):
        to = pl.ds(pl.multiple_of(k * r_size, r_size), r_size)
        came = pl.ds(pl.multiple_of(me_x * out_cols + k * r_size, r_size), r_size)
        wd2[me_x, to, :] = wd[came, :]
        return 0

    lax.fori_loop(0, 7, own_part, 0)
    ring_a(1, 4)
    share_pair(1, 3)
    gl_pair(2)
    ring_b(1, 4)

    def w2_pass(j, _):
        for i in range(n_mp - 1):
            ref = w2_rows(i, j, core)
            remote(ref, ref, w2_send.at[j], w2_recv.at[i, j], {"mp": x_peers[i][0]}).wait_recv()
            w2_share(i, j, core).start()
        return 0

    def middle(s, _):
        gl_pair(s - 2)
        ring_step(1, s, lambda: share_pair(1, s - 1))
        return 0

    lax.fori_loop(5, 7, middle, 0)
    gl_pair(5)
    for i in range(n_mp - 1):
        ref = gain_all.at[x_peers[i][1]]
        remote(ref, ref, ga_send.at[i], ga_recv.at[i], {"mp": x_peers[i][0]}).wait_recv()
    for b in range(n_mp):
        gain_b[b * lat_cols : (b + 1) * lat_cols, :] = jnp.broadcast_to(gain_all[b], (n_tok, lat_cols)).T
    for i in range(n_mp - 1):
        lr_copy(i, x_peers[i][1]).wait_recv()
    squares = jnp.zeros((1, n_tok), F32)
    for b in range(n_mp):
        value = lr_t[b * lat_cols : (b + 1) * lat_cols, :]
        squares = squares + jnp.sum(value * value, axis=0, keepdims=True)
    root[...] = jnp.sqrt(squares / lat + 1e-06)
    for b in range(n_mp):
        at = slice(b * lat_cols, (b + 1) * lat_cols)
        lat_t[at, :] = (lr_t[at, :] / root[...] * gain_b[at, :]).astype(BF16)

    compute([z], gl=False, first=True)
    q_pair(1)
    ring_a(1, 7)
    share_pair(1, 6)
    q_pair(2)
    q_pair(3)
    ring_b(1, 7)
    gl_pair(6)
    q_pair(4)
    lax.fori_loop(0, per_x, w2_pass, 0)
    for way in (0, 1):
        bz = (left, right)[way](half - 1)
        y_copy(1, bz, part_c).wait_recv()
        far_copy(way).start()
        c_copy(1, bz, core).start()
    z_copy(1, 0, far, part_a).wait_recv()
    z_copy(1, 1, far, part_b).wait_recv()
    far_share(0, core).start()
    gl_pair(half - 1)
    q_pair(5)
    z_copy(1, 0, far, part_c).wait_recv()
    far_share(1, core).start()
    q_pair(6)
    far_share(0, 1 - core).wait_recv()
    far_share(1, 1 - core).wait_recv()
    compute([far], q=False)
    q_pair(7)
    compute([far], gl=False, final=True)
    q_store = pltpu.make_async_copy(q_out, q_h, out_sem.at[0])
    q_store.start()

    for kind in (0, 1):
        for part in (part_a, part_b):
            for way in (0, 1):
                z_copy(kind, way, z, part).wait_send()
        c_copy(kind, z, core).wait_send()

        def drain(s, _, kind=kind):
            lz, rz = left(s), right(s)
            z_copy(kind, 0, lz, part_a).wait_send()
            z_copy(kind, 1, rz, part_b).wait_send()

            @pl.when(s < half - 1)
            def _():
                z_copy(kind, 1, rz, part_a).wait_send()
                z_copy(kind, 0, lz, part_b).wait_send()

            for bz in (lz, rz):
                y_copy(kind, bz, part_a).wait_send()
                c_copy(kind, bz, core).wait_send()
            return 0

        lax.fori_loop(1, half, drain, 0)
    y_copy(0, far, part_a).wait_send()
    c_copy(0, far, core).wait_send()
    for i in range(2):
        far_copy(i).wait_send()
        far_share(i, core).wait_send()
    for i in range(n_mp - 1):
        gain_copy(i).wait_send()
        lr_copy(i, me_x).wait_send()
        for j in range(per_x):
            w2_share(i, j, core).wait_send()

    def drain_w2(bz, _):
        @pl.when(bz // per_x != me_x)
        def _():
            w2_copy(bz).wait_send()

        return 0

    lax.fori_loop(0, n_z, drain_w2, 0)

    def wait_gl(bz, _):
        for i in range(n_mp - 1):
            gl_copy(i, bz).wait_send()
            gl_copy(i, bz).wait_recv()
        return 0

    lax.fori_loop(0, n_z, wait_gl, 0)
    inner = jnp.zeros((1, n_tok), F32)
    for b in range(n_mp):
        at = slice(b * lat_cols, (b + 1) * lat_cols)
        total = own_gl[at, :]
        for i in range(n_mp - 1):
            total = total + peer_gl[i, at, :].astype(F32)
        total = total * gain_b[at, :]
        own_gl[at, :] = total
        inner = inner + jnp.sum(total * lr_t[at, :], axis=0, keepdims=True)
    scale = inner / (lat * root[...] * root[...] * root[...])
    for b in range(n_mp):
        at = slice(b * lat_cols, (b + 1) * lat_cols)
        grad_raw[b] = (own_gl[at, :] / root[...] - lr_t[at, :] * scale).T.astype(BF16)
    for i in range(n_mp - 1):
        for j in range(per_x):
            w2_share(i, j, 1 - core).wait_recv()

    for k in range(7):
        at = slice(k * r_size, (k + 1) * r_size)
        total = jnp.zeros((n_tok, r_size), F32)
        for b in range(n_mp):
            total = total + lax.dot_general(
                grad_raw[b], wd2[b, at, :], (((1,), (1,)), ((), ())), preferred_element_type=F32
            )
        gt_out[:, at] = total.astype(BF16)
    gt_store = pltpu.make_async_copy(gt_out, gt_h, out_sem.at[1])
    gt_store.start()

    q_store.wait()
    gt_store.wait()


def write_kernel(q_in, gt_in, q_h, gt_h, q_hold, gt_hold, in_sem, out_sem):
    n_tok = q_in.shape[0]
    quarter = n_tok // 4
    pairs = [(q_in, q_hold, q_h, slice(k * quarter, (k + 1) * quarter)) for k in range(4)]
    pairs.append((gt_in, gt_hold, gt_h, slice(0, n_tok)))

    def load(k):
        src, hold, _, at = pairs[k]
        return pltpu.make_async_copy(src.at[at, :], hold.at[at, :], in_sem.at[k])

    def store(k):
        _, hold, dst, at = pairs[k]
        return pltpu.make_async_copy(hold.at[at, :], dst.at[at, :], out_sem.at[k])

    for k in range(len(pairs)):
        load(k).start()
    for k in range(len(pairs)):
        load(k).wait()
        store(k).start()
    for k in range(len(pairs)):
        store(k).wait()


def body(tokens, w_down, gain, w_up, head_counts, cotangent):
    n_dp, n_mp = lax.axis_size("dp"), lax.axis_size("mp")
    n_z = n_dp // 2
    n_tok, width = tokens.shape
    up_rows, cols = w_up.shape
    lat_cols = w_down.shape[1]
    lat = lat_cols * n_mp
    out_cols = width // n_mp
    dma = pltpu.SemaphoreType.DMA
    anywhere = pl.BlockSpec(memory_space=pl.ANY)
    peers = n_mp - 1
    queries, grad_tokens = pl.pallas_call(
        kernel,
        out_shape=(
            jax.ShapeDtypeStruct((n_tok, cols), BF16),
            jax.ShapeDtypeStruct((n_tok, out_cols), BF16),
        ),
        in_specs=[
            anywhere,
            anywhere,
            anywhere,
            anywhere,
            anywhere,
            anywhere,
        ],
        out_specs=(anywhere, anywhere),
        scratch_shapes=[
            pltpu.VMEM((n_tok, width), BF16),
            pltpu.VMEM((width, lat_cols), BF16),
            pltpu.VMEM((n_mp, out_cols, lat_cols), BF16),
            pltpu.VMEM((lat, cols), BF16),
            pltpu.VMEM((n_tok, cols), BF16),
            pltpu.VMEM((cols, n_tok), BF16),
            pltpu.VMEM((lat, n_tok), F32),
            pltpu.VMEM((lat, n_tok), BF16),
            pltpu.VMEM((lat, n_tok), F32),
            pltpu.VMEM((n_mp, 1, lat_cols), F32),
            pltpu.VMEM((lat, n_tok), F32),
            pltpu.VMEM((lat, n_tok), BF16),
            pltpu.VMEM((peers, lat, n_tok), BF16),
            pltpu.VMEM((n_mp, n_tok, lat_cols), BF16),
            pltpu.VMEM((n_tok, cols), F32),
            pltpu.VMEM((n_tok, cols), BF16),
            pltpu.VMEM((n_tok, out_cols), BF16),
            pltpu.VMEM((1, n_tok), F32),
            dma((6,)),
            dma((2,)),
            dma((2, 2, 3, n_z)),
            dma((2, 3, n_z)),
            dma((2, n_z)),
            dma((2, n_z)),
            dma((2, n_z)),
            dma((peers,)),
            dma((peers,)),
            dma((peers,)),
            dma((peers,)),
            dma((n_z,)),
            dma((peers, n_z // n_mp)),
            dma((peers, n_z // n_mp)),
            dma((peers, n_z // n_mp)),
            dma((peers, n_z)),
            dma((peers, n_z)),
            dma((2,)),
            dma((2,)),
            dma((2,)),
            pltpu.VMEM(gain.shape, F32),
            pltpu.SMEM(head_counts.shape, jnp.int32),
        ],
        compiler_params=pltpu.CompilerParams(
            collective_id=0, has_side_effects=True, vmem_limit_bytes=60 * 1024 * 1024
        ),
        name="gather_and_project",
    )(tokens, w_down, gain, w_up, head_counts, cotangent)
    return pl.pallas_call(
        write_kernel,
        out_shape=(
            jax.ShapeDtypeStruct((n_tok, cols), BF16),
            jax.ShapeDtypeStruct((n_tok, out_cols), BF16),
        ),
        in_specs=[anywhere, anywhere],
        out_specs=(anywhere, anywhere),
        scratch_shapes=[
            pltpu.VMEM((n_tok, cols), BF16),
            pltpu.VMEM((n_tok, out_cols), BF16),
            dma((5,)),
            dma((5,)),
        ],
        name="write_outputs",
    )(queries, grad_tokens)


def solution(mesh):
    in_specs = (
        P(("groups", "dp"), None),
        P("dp", "mp"),
        P("mp"),
        P("dp", "mp"),
        P(),
        P(("groups", "dp"), "mp"),
    )
    out_specs = (P(("groups", "dp"), "mp"), P(("groups", "dp"), "mp"))
    return jax.shard_map(body, mesh=mesh, in_specs=in_specs, out_specs=out_specs, check_vma=False)
```

```python
import functools

import jax
import jax.numpy as jnp
from jax import lax
from jax.experimental import pallas as pl
from jax.experimental.pallas import tpu as pltpu
from jax.sharding import PartitionSpec as P

HD = 192
MESH = pl.DeviceIdType.MESH
F32 = jnp.float32
BF16 = jnp.bfloat16


def kernel(
    tok_h, wd_h, gain_h, wu_h, heads_h, cot_h, q_h, gt_h,
    tok, wd, wd2, wu, cot, cot_t, lr_t, lat_t, gain_b, gain_all,
    own_gl, send_gl, peer_gl, grad_raw, q_acc, q_out, gt_out, root,
    load_sem, out_sem, z_send, z_recv, y_send, c_send, c_recv,
    lr_send, lr_recv, ga_send, ga_recv, w2_send, w2_recv, w2c_send, w2c_recv, gl_send, gl_recv,
    far_send, gain_ref, heads_ref,
):
    n_dp, n_mp = lax.axis_size("dp"), lax.axis_size("mp")
    n_z = n_dp // 2
    half = n_z // 2
    me_g, me_dp, me_x = lax.axis_index("groups"), lax.axis_index("dp"), lax.axis_index("mp")
    z, core = me_dp // 2, me_dp % 2
    plane = me_g % 2
    partner = me_g + 1 - 2 * plane
    after, before = (me_dp + 2) % n_dp, (me_dp + n_dp - 2) % n_dp
    sibling = me_dp + 1 - 2 * core

    up_rows, cols = wu_h.shape
    down_rows, lat_cols = wd_h.shape
    n_tok, width = tok_h.shape
    lat = lat_cols * n_mp
    out_cols = width // n_mp
    rows3, cols3 = up_rows // 3, lat_cols // 3
    part_a, part_b, part_c = 2 * plane, 1, 2 * (1 - plane)

    def block(kind, bz, bc):
        if kind == 0:
            return wd.at[pl.ds(pl.multiple_of((2 * bz + bc) * down_rows, down_rows), down_rows), :]
        return wu.at[pl.ds(pl.multiple_of((2 * bz + bc) * up_rows, up_rows), up_rows), :]

    def piece(kind, bz, part):
        if kind == 0:
            rows = pl.ds(pl.multiple_of((2 * bz + core) * down_rows, down_rows), down_rows)
            return wd.at[rows, pl.ds(pl.multiple_of(part * cols3, cols3), cols3)]
        return wu.at[pl.ds(pl.multiple_of((2 * bz + core) * up_rows + part * rows3, rows3), rows3), :]

    def remote(src, dst, send, recv, where):
        return pltpu.make_async_remote_copy(
            src_ref=src, dst_ref=dst, send_sem=send, recv_sem=recv, device_id=where, device_id_type=MESH
        )

    def z_copy(kind, way, bz, part):
        ref = piece(kind, bz, part)
        return remote(
            ref, ref, z_send.at[kind], z_recv.at[kind, part, bz], {"dp": (after, before)[way]}
        )

    def y_copy(kind, bz, part):
        ref = piece(kind, bz, part)
        return remote(ref, ref, y_send.at[kind], z_recv.at[kind, part, bz], {"groups": partner})

    def c_copy(kind, bz, bc):
        ref = block(kind, bz, bc)
        return remote(ref, ref, c_send.at[kind], c_recv.at[bz if kind else n_z], {"dp": sibling})

    def c_part(bz, which):
        base = (2 * bz + core) * up_rows
        if which == 0:
            rows = pl.ds(pl.multiple_of(base + plane * rows3, rows3), 2 * rows3)
        else:
            rows = pl.ds(pl.multiple_of(base + part_c * rows3, rows3), rows3)
        ref = wu.at[rows, :]
        return remote(ref, ref, c_send.at[1], c_recv.at[bz], {"dp": sibling})

    def left(s):
        return (z + n_z - s) % n_z

    def right(s):
        return (z + s) % n_z

    own_down = pltpu.make_async_copy(wd_h, block(0, z, core), load_sem.at[0])
    own_up = pltpu.make_async_copy(wu_h, block(1, z, core), load_sem.at[1])
    load_cot = pltpu.make_async_copy(cot_h, cot, load_sem.at[2])
    load_tok = pltpu.make_async_copy(tok_h, tok, load_sem.at[3])
    own_down.start()
    own_up.start()
    load_gain = pltpu.make_async_copy(gain_h, gain_ref, load_sem.at[4])
    load_heads = pltpu.make_async_copy(heads_h, heads_ref, load_sem.at[5])
    load_gain.start()
    load_heads.start()
    load_cot.start()
    load_tok.start()

    barrier = pltpu.get_barrier_semaphore()
    others = [{"dp": after}, {"dp": before}, {"dp": sibling}, {"groups": partner}]
    others += [{"mp": (me_x + i) % n_mp} for i in range(1, n_mp)]
    for where in others:
        pl.semaphore_signal(barrier, inc=1, device_id=where, device_id_type=MESH)
    pl.semaphore_wait(barrier, len(others))

    def send_own_down():
        for part in (part_a, part_b):
            for way in (0, 1):
                z_copy(0, way, z, part).start()
        c_copy(0, z, core).start()

    wide = cols // 3

    def send_own_up(j):
        part = jnp.where(j < 3, part_a, part_b)
        rows = pl.ds(pl.multiple_of((2 * z + core) * up_rows + part * rows3, rows3), rows3)
        ref = wu.at[rows, pl.ds(pl.multiple_of((j % 3) * wide, 128), wide)]
        for way in (0, 1):
            remote(
                ref, ref, z_send.at[1], z_recv.at[1, part, z], {"dp": (after, before)[way]}
            ).start()

    def ring_a(kind, s):
        lz, rz = left(s), right(s)
        z_copy(kind, 0, lz, part_a).wait_recv()
        z_copy(kind, 0, lz, part_a).start()
        y_copy(kind, lz, part_a).start()
        z_copy(kind, 1, rz, part_a).wait_recv()

        @pl.when(s < half - 1)
        def _():
            z_copy(kind, 1, rz, part_a).start()

        y_copy(kind, rz, part_a).start()

    def ring_b(kind, s):
        lz, rz = left(s), right(s)
        z_copy(kind, 0, lz, part_b).wait_recv()

        @pl.when(s < half - 1)
        def _():
            z_copy(kind, 0, lz, part_b).start()

        z_copy(kind, 1, rz, part_b).wait_recv()
        z_copy(kind, 1, rz, part_b).start()
        if kind == 1:
            c_part(lz, 0).start()
            c_part(rz, 0).start()

    def ring_step(kind, s, between):
        ring_a(kind, s)
        between()
        ring_b(kind, s)

    far = right(half)

    x_peers = [((me_x + i) % n_mp, (me_x + n_mp - i) % n_mp) for i in range(1, n_mp)]
    per_x = n_z // n_mp

    def w2_at(owner, j, bc):
        return wd2.at[owner, pl.ds(pl.multiple_of((2 * j + bc) * down_rows, down_rows), down_rows), :]

    def w2_copy(bz):
        to = bz // per_x
        j = bz - to * per_x
        return remote(block(0, bz, core), w2_at(me_x, j, core), w2_send.at[0], w2_recv.at[0], {"mp": to})

    def pass_on(bz):
        @pl.when(bz // per_x != me_x)
        def _():
            w2_copy(bz).start()

    def w2_rows(i, j, bc):
        return w2_at(x_peers[i][1], j, bc)

    def w2_share(i, j, bc):
        ref = w2_rows(i, j, bc)
        return remote(ref, ref, w2c_send.at[0], w2c_recv.at[0], {"dp": sibling})

    def share(kind, bz):
        y_copy(kind, bz, part_c).wait_recv()
        if kind == 0:
            c_copy(0, bz, core).start()
            pass_on(bz)
        else:
            c_part(bz, 1).start()

    def share_pair(kind, s):
        share(kind, left(s))
        share(kind, right(s))

    def wait_sibling(kind, bz):
        c_copy(kind, bz, 1 - core).wait_recv()

    n_lane_tiles = cols // 128
    cut = n_lane_tiles * 2 // 3 * 128

    def far_part(bz):
        return pl.ds(pl.multiple_of((2 * bz + core) * up_rows + part_c * rows3, rows3), rows3)

    def far_copy(way):
        bz = (left, right)[way](half - 1)
        ref = wu.at[far_part(bz), (slice(0, cut), slice(cut, cols))[way]]
        return remote(ref, ref, far_send.at[0], z_recv.at[1, part_c, bz], {"dp": (after, before)[way]})

    lane1 = lax.broadcasted_iota(jnp.int32, (1, 128), 1)

    own_down.wait()
    send_own_down()
    own_up.wait()
    send_own_up(0)
    pass_on(z)
    c_copy(1, z, core).start()
    def gain_copy(i):
        return remote(
            gain_all.at[me_x], gain_all.at[me_x], ga_send.at[0], ga_recv.at[0], {"mp": x_peers[i][0]}
        )

    load_gain.wait()
    load_heads.wait()
    held = jnp.int32(0)
    for i in range(n_mp):
        held = held + jnp.where(me_x == i, heads_ref[i], 0)
    kept = held * HD
    gain_all[me_x] = gain_ref[...].reshape(1, lat_cols)
    load_cot.wait()
    n_blocks = cols // 128
    per_step = -(-n_blocks // (half - 1))

    def turn(j, _):
        at = pl.ds(pl.multiple_of(j * 128, 128), 128)
        value = jnp.where(lane1 + j * 128 < kept, cot[:, at], jnp.zeros((), BF16))
        cot_t[at, :] = value.T
        return 0

    def down_step(s, _):
        def between():
            @pl.when(s > 2)
            def _():
                share_pair(0, s - 2)

        ring_step(0, s, between)

        @pl.when(s <= 5)
        def _():
            send_own_up(s)

        @pl.when(s == 4)
        def _():
            z_copy(1, 0, left(1), part_a).wait_recv()
            y_copy(1, left(1), part_a).start()

        @pl.when(s == 5)
        def _():
            z_copy(1, 1, right(1), part_a).wait_recv()
            y_copy(1, right(1), part_a).start()

        @pl.when(s == 6)
        def _():
            z_copy(1, 0, left(1), part_a).start()
            z_copy(1, 1, right(1), part_a).start()

        lax.fori_loop((s - 1) * per_step, jnp.minimum(s * per_step, n_blocks), turn, 0)
        return 0

    lax.fori_loop(1, half, down_step, 0)
    z_copy(1, 0, left(1), part_b).wait_recv()
    z_copy(1, 0, left(1), part_b).start()
    z_copy(1, 1, right(1), part_b).wait_recv()
    z_copy(1, 1, right(1), part_b).start()
    c_part(left(1), 0).start()
    c_part(right(1), 0).start()
    for i in range(n_mp - 1):
        gain_copy(i).start()
    z_copy(0, 0, far, part_a).wait_recv()
    y_copy(0, far, part_a).start()
    z_copy(0, 1, far, part_b).wait_recv()
    ring_a(1, 2)
    share_pair(0, half - 2)
    share_pair(0, half - 1)
    share(0, far)
    ring_b(1, 2)
    load_tok.wait()

    from_sibling = wd.at[pl.ds(0, n_z * down_rows), :]
    remote(from_sibling, from_sibling, c_send.at[0], c_recv.at[n_z], {"dp": sibling}).wait_recv()

    k_size = width // 7

    def latent_part(k, total):
        at = pl.ds(pl.multiple_of(k * k_size, k_size), k_size)
        return total + jnp.dot(tok[:, at], wd[at, :], preferred_element_type=F32)

    latent_raw = lax.fori_loop(0, 7, latent_part, jnp.zeros((n_tok, lat_cols), F32))

    def lat_rows(owner):
        return pl.ds(pl.multiple_of(owner * lat_cols, lat_cols), lat_cols)

    lr_t[lat_rows(me_x), :] = latent_raw.T

    def lr_copy(i, owner):
        ref = lr_t.at[lat_rows(owner), :]
        return remote(ref, ref, lr_send.at[0], lr_recv.at[0], {"mp": x_peers[i][0]})

    for i in range(n_mp - 1):
        lr_copy(i, me_x).start()
    z_rows = 2 * up_rows

    def rows_of(bz):
        return pl.ds(pl.multiple_of(bz * z_rows, z_rows), z_rows)

    def gl_copy(i, bz):
        return remote(
            send_gl.at[rows_of(bz), :], peer_gl.at[i, rows_of(bz), :],
            gl_send.at[0], gl_recv.at[0], {"mp": x_peers[i][0]},
        )

    def publish(bz, value):
        own_gl[rows_of(bz), :] = value
        send_gl[rows_of(bz), :] = value.astype(BF16)

    def send_blocks(zs):
        for bz in zs:
            for i in range(n_mp - 1):
                gl_copy(i, bz).start()

    tiles = [(off, min(256, wide - off)) for off in range(0, wide, 256)]

    def compute(zs, gl=True, q=True, first=False, final=False):
        if q:
            one = jnp.concatenate([lat_t[rows_of(bz), :] for bz in zs], axis=0).T

        def step(c, total):
            for off, size in tiles:
                at = pl.ds(pl.multiple_of(c * wide + off, 128), size)
                tile = jnp.concatenate([wu[rows_of(bz), at] for bz in zs], axis=0)
                if gl:
                    total = total + jnp.dot(tile, cot_t[at, :], preferred_element_type=F32)
                if q:
                    value = jnp.dot(one, tile, preferred_element_type=F32)
                    if not first:
                        value = value + q_acc[:, at]
                    if final:
                        lane = lax.broadcasted_iota(jnp.int32, (1, size), 1) + (c * wide + off)
                        q_out[:, at] = jnp.where(lane < kept, value, 0.0).astype(BF16)
                    else:
                        q_acc[:, at] = value
            return total

        start = jnp.zeros((z_rows * len(zs), n_tok), F32) if gl else 0
        total = lax.fori_loop(0, 3, step, start)
        if gl:
            for k, bz in enumerate(zs):
                publish(bz, total[k * z_rows : (k + 1) * z_rows])
            send_blocks(zs)

    def pair(s):
        return [left(s), right(s)]

    def gl_pair(s):
        for bz in pair(s):
            wait_sibling(1, bz)
        compute(pair(s), q=False)

    def q_pair(s):
        compute(pair(s), gl=False)

    ring_a(1, 3)
    share_pair(1, 1)
    share_pair(1, 2)
    wait_sibling(1, z)
    compute([z], q=False)
    ring_b(1, 3)
    gl_pair(1)
    r_size = out_cols // 7

    def own_part(k, _):
        to = pl.ds(pl.multiple_of(k * r_size, r_size), r_size)
        came = pl.ds(pl.multiple_of(me_x * out_cols + k * r_size, r_size), r_size)
        wd2[me_x, to, :] = wd[came, :]
        return 0

    lax.fori_loop(0, 7, own_part, 0)
    ring_a(1, 4)
    share_pair(1, 3)
    gl_pair(2)
    ring_b(1, 4)

    def whole(ref, send, recv):
        return remote(ref, ref, send.at[0], recv.at[0], {"dp": sibling})

    w2_bytes = wd.at[pl.ds(0, (n_mp - 1) * per_x * down_rows), :]

    def w2_pass(j, _):
        for i in range(n_mp - 1):
            w2_share(i, j, core).start()
        return 0

    def middle(s, _):
        gl_pair(s - 2)
        ring_step(1, s, lambda: share_pair(1, s - 1))
        return 0

    lax.fori_loop(5, 7, middle, 0)
    gl_pair(5)
    gain_bytes = gain_all.at[pl.ds(0, n_mp - 1)]
    lat_bytes = lr_t.at[pl.ds(0, (n_mp - 1) * lat_cols), :]
    whole(gain_bytes, ga_send, ga_recv).wait_recv()
    for b in range(n_mp):
        gain_b[b * lat_cols : (b + 1) * lat_cols, :] = jnp.broadcast_to(gain_all[b], (n_tok, lat_cols)).T
    whole(lat_bytes, lr_send, lr_recv).wait_recv()
    squares = jnp.zeros((1, n_tok), F32)
    for b in range(n_mp):
        value = lr_t[b * lat_cols : (b + 1) * lat_cols, :]
        squares = squares + jnp.sum(value * value, axis=0, keepdims=True)
    root[...] = jnp.sqrt(squares / lat + 1e-06)
    for b in range(n_mp):
        at = slice(b * lat_cols, (b + 1) * lat_cols)
        lat_t[at, :] = (lr_t[at, :] / root[...] * gain_b[at, :]).astype(BF16)

    compute([z], gl=False, first=True)
    q_pair(1)
    ring_a(1, 7)
    share_pair(1, 6)
    q_pair(2)
    q_pair(3)
    ring_b(1, 7)
    gl_pair(6)
    q_pair(4)
    whole(w2_bytes, w2_send, w2_recv).wait_recv()
    lax.fori_loop(0, per_x, w2_pass, 0)
    for way in (0, 1):
        bz = (left, right)[way](half - 1)
        y_copy(1, bz, part_c).wait_recv()
        far_copy(way).start()
        c_part(bz, 1).start()
    z_copy(1, 0, far, part_a).wait_recv()
    z_copy(1, 1, far, part_b).wait_recv()
    c_part(far, 0).start()
    gl_pair(half - 1)
    q_pair(5)
    z_copy(1, 0, far, part_c).wait_recv()
    c_part(far, 1).start()
    q_pair(6)
    wait_sibling(1, far)
    compute([far], q=False)
    q_pair(7)
    compute([far], gl=False, final=True)
    q_store = pltpu.make_async_copy(q_out, q_h, out_sem.at[0])
    q_store.start()

    thirds = 2 * (n_z - 1)
    sends = [
        (wd.at[pl.ds(0, thirds * down_rows // 3), :], z_send.at[0]),
        (wu.at[pl.ds(0, thirds * rows3), :], z_send.at[1]),
        (wd.at[pl.ds(0, (n_z - 1) * down_rows // 3), :], y_send.at[0]),
        (wu.at[pl.ds(0, (n_z - 2) * rows3), :], y_send.at[1]),
        (wd.at[pl.ds(0, n_z * down_rows), :], c_send.at[0]),
        (wu.at[pl.ds(0, n_z * up_rows), :], c_send.at[1]),
        (wu.at[pl.ds(0, rows3), :], far_send.at[0]),
        (gain_bytes, ga_send.at[0]),
        (lat_bytes, lr_send.at[0]),
        (w2_bytes, w2_send.at[0]),
        (w2_bytes, w2c_send.at[0]),
        (peer_gl, gl_send.at[0]),
    ]
    for ref, sem in sends:
        remote(ref, ref, sem, c_recv.at[n_z], {"dp": sibling}).wait_send()
    whole(peer_gl, gl_send, gl_recv).wait_recv()
    inner = jnp.zeros((1, n_tok), F32)
    for b in range(n_mp):
        at = slice(b * lat_cols, (b + 1) * lat_cols)
        total = own_gl[at, :]
        for i in range(n_mp - 1):
            total = total + peer_gl[i, at, :].astype(F32)
        total = total * gain_b[at, :]
        own_gl[at, :] = total
        inner = inner + jnp.sum(total * lr_t[at, :], axis=0, keepdims=True)
    scale = inner / (lat * root[...] * root[...] * root[...])
    for b in range(n_mp):
        at = slice(b * lat_cols, (b + 1) * lat_cols)
        grad_raw[b] = (own_gl[at, :] / root[...] - lr_t[at, :] * scale).T.astype(BF16)
    whole(w2_bytes, w2c_send, w2c_recv).wait_recv()

    for k in range(7):
        at = slice(k * r_size, (k + 1) * r_size)
        total = jnp.zeros((n_tok, r_size), F32)
        for b in range(n_mp):
            total = total + lax.dot_general(
                grad_raw[b], wd2[b, at, :], (((1,), (1,)), ((), ())), preferred_element_type=F32
            )
        gt_out[:, at] = total.astype(BF16)
    gt_store = pltpu.make_async_copy(gt_out, gt_h, out_sem.at[1])
    gt_store.start()

    q_store.wait()
    gt_store.wait()


def write_kernel(q_in, gt_in, q_h, gt_h, q_hold, gt_hold, in_sem, out_sem):
    n_tok = q_in.shape[0]
    quarter = n_tok // 4
    pairs = [(q_in, q_hold, q_h, slice(k * quarter, (k + 1) * quarter)) for k in range(4)]
    pairs.append((gt_in, gt_hold, gt_h, slice(0, n_tok)))

    def load(k):
        src, hold, _, at = pairs[k]
        return pltpu.make_async_copy(src.at[at, :], hold.at[at, :], in_sem.at[k])

    def store(k):
        _, hold, dst, at = pairs[k]
        return pltpu.make_async_copy(hold.at[at, :], dst.at[at, :], out_sem.at[k])

    for k in range(len(pairs)):
        load(k).start()
    for k in range(len(pairs)):
        load(k).wait()
        store(k).start()
    for k in range(len(pairs)):
        store(k).wait()


def body(tokens, w_down, gain, w_up, head_counts, cotangent):
    n_dp, n_mp = lax.axis_size("dp"), lax.axis_size("mp")
    n_z = n_dp // 2
    n_tok, width = tokens.shape
    up_rows, cols = w_up.shape
    lat_cols = w_down.shape[1]
    lat = lat_cols * n_mp
    out_cols = width // n_mp
    dma = pltpu.SemaphoreType.DMA
    anywhere = pl.BlockSpec(memory_space=pl.ANY)
    peers = n_mp - 1
    queries, grad_tokens = pl.pallas_call(
        kernel,
        out_shape=(
            jax.ShapeDtypeStruct((n_tok, cols), BF16),
            jax.ShapeDtypeStruct((n_tok, out_cols), BF16),
        ),
        in_specs=[
            anywhere,
            anywhere,
            anywhere,
            anywhere,
            anywhere,
            anywhere,
        ],
        out_specs=(anywhere, anywhere),
        scratch_shapes=[
            pltpu.VMEM((n_tok, width), BF16),
            pltpu.VMEM((width, lat_cols), BF16),
            pltpu.VMEM((n_mp, out_cols, lat_cols), BF16),
            pltpu.VMEM((lat, cols), BF16),
            pltpu.VMEM((n_tok, cols), BF16),
            pltpu.VMEM((cols, n_tok), BF16),
            pltpu.VMEM((lat, n_tok), F32),
            pltpu.VMEM((lat, n_tok), BF16),
            pltpu.VMEM((lat, n_tok), F32),
            pltpu.VMEM((n_mp, 1, lat_cols), F32),
            pltpu.VMEM((lat, n_tok), F32),
            pltpu.VMEM((lat, n_tok), BF16),
            pltpu.VMEM((peers, lat, n_tok), BF16),
            pltpu.VMEM((n_mp, n_tok, lat_cols), BF16),
            pltpu.VMEM((n_tok, cols), F32),
            pltpu.VMEM((n_tok, cols), BF16),
            pltpu.VMEM((n_tok, out_cols), BF16),
            pltpu.VMEM((1, n_tok), F32),
            dma((6,)),
            dma((2,)),
            dma((2,)),
            dma((2, 3, n_z)),
            dma((2,)),
            dma((2,)),
            dma((n_z + 1,)),
            dma((1,)),
            dma((1,)),
            dma((1,)),
            dma((1,)),
            dma((1,)),
            dma((1,)),
            dma((1,)),
            dma((1,)),
            dma((1,)),
            dma((1,)),
            dma((1,)),
            pltpu.VMEM(gain.shape, F32),
            pltpu.SMEM(head_counts.shape, jnp.int32),
        ],
        compiler_params=pltpu.CompilerParams(
            collective_id=0, has_side_effects=True, vmem_limit_bytes=60 * 1024 * 1024
        ),
        name="gather_and_project",
    )(tokens, w_down, gain, w_up, head_counts, cotangent)
    return pl.pallas_call(
        write_kernel,
        out_shape=(
            jax.ShapeDtypeStruct((n_tok, cols), BF16),
            jax.ShapeDtypeStruct((n_tok, out_cols), BF16),
        ),
        in_specs=[anywhere, anywhere],
        out_specs=(anywhere, anywhere),
        scratch_shapes=[
            pltpu.VMEM((n_tok, cols), BF16),
            pltpu.VMEM((n_tok, out_cols), BF16),
            dma((5,)),
            dma((5,)),
        ],
        name="write_outputs",
    )(queries, grad_tokens)


def solution(mesh):
    in_specs = (
        P(("groups", "dp"), None),
        P("dp", "mp"),
        P("mp"),
        P("dp", "mp"),
        P(),
        P(("groups", "dp"), "mp"),
    )
    out_specs = (P(("groups", "dp"), "mp"), P(("groups", "dp"), "mp"))
    return jax.shard_map(body, mesh=mesh, in_specs=in_specs, out_specs=out_specs, check_vma=False)
```

```python
import functools

import jax
import jax.numpy as jnp
from jax import lax
from jax.experimental import pallas as pl
from jax.experimental.pallas import tpu as pltpu
from jax.sharding import PartitionSpec as P

HD = 192
MESH = pl.DeviceIdType.MESH
F32 = jnp.float32
BF16 = jnp.bfloat16


def kernel(
    tok_h, wd_h, gain_h, wu_h, heads_h, cot_h, q_h, gt_h,
    tok, wd, wd2, wu, cot, cot_t, lr_t, lat_t, gain_b, gain_all,
    own_gl, send_gl, peer_gl, grad_raw, q_acc, q_out, gt_out, root,
    load_sem, out_sem, z_send, z_recv, y_send, c_send, c_recv,
    lr_send, lr_recv, ga_send, ga_recv, w2_send, w2_recv, w2c_send, w2c_recv, gl_send, gl_recv,
    far_send, gain_ref, heads_ref,
):
    n_dp, n_mp = lax.axis_size("dp"), lax.axis_size("mp")
    n_z = n_dp // 2
    half = n_z // 2
    me_g, me_dp, me_x = lax.axis_index("groups"), lax.axis_index("dp"), lax.axis_index("mp")
    z, core = me_dp // 2, me_dp % 2
    plane = me_g % 2
    partner = me_g + 1 - 2 * plane
    after, before = (me_dp + 2) % n_dp, (me_dp + n_dp - 2) % n_dp
    sibling = me_dp + 1 - 2 * core

    up_rows, cols = wu_h.shape
    down_rows, lat_cols = wd_h.shape
    n_tok, width = tok_h.shape
    lat = lat_cols * n_mp
    out_cols = width // n_mp
    rows3, cols3 = up_rows // 3, lat_cols // 3
    part_a, part_b, part_c = 2 * plane, 1, 2 * (1 - plane)

    def block(kind, bz, bc):
        if kind == 0:
            return wd.at[pl.ds(pl.multiple_of((2 * bz + bc) * down_rows, down_rows), down_rows), :]
        return wu.at[pl.ds(pl.multiple_of((2 * bz + bc) * up_rows, up_rows), up_rows), :]

    def piece(kind, bz, part):
        if kind == 0:
            rows = pl.ds(pl.multiple_of((2 * bz + core) * down_rows, down_rows), down_rows)
            return wd.at[rows, pl.ds(pl.multiple_of(part * cols3, cols3), cols3)]
        return wu.at[pl.ds(pl.multiple_of((2 * bz + core) * up_rows + part * rows3, rows3), rows3), :]

    def remote(src, dst, send, recv, where):
        return pltpu.make_async_remote_copy(
            src_ref=src, dst_ref=dst, send_sem=send, recv_sem=recv, device_id=where, device_id_type=MESH
        )

    def z_copy(kind, way, bz, part):
        ref = piece(kind, bz, part)
        return remote(
            ref, ref, z_send.at[kind], z_recv.at[kind, part, bz], {"dp": (after, before)[way]}
        )

    def y_copy(kind, bz, part):
        ref = piece(kind, bz, part)
        return remote(ref, ref, y_send.at[kind], z_recv.at[kind, part, bz], {"groups": partner})

    def c_copy(kind, bz, bc):
        ref = block(kind, bz, bc)
        return remote(ref, ref, c_send.at[kind], c_recv.at[bz if kind else n_z], {"dp": sibling})

    def c_part(bz, which):
        base = (2 * bz + core) * up_rows
        if which == 0:
            rows = pl.ds(pl.multiple_of(base + plane * rows3, rows3), 2 * rows3)
        else:
            rows = pl.ds(pl.multiple_of(base + part_c * rows3, rows3), rows3)
        ref = wu.at[rows, :]
        return remote(ref, ref, c_send.at[1], c_recv.at[bz], {"dp": sibling})

    def left(s):
        return (z + n_z - s) % n_z

    def right(s):
        return (z + s) % n_z

    own_down = pltpu.make_async_copy(wd_h, block(0, z, core), load_sem.at[0])
    own_up = pltpu.make_async_copy(wu_h, block(1, z, core), load_sem.at[1])
    load_cot = pltpu.make_async_copy(cot_h, cot, load_sem.at[2])
    load_tok = pltpu.make_async_copy(tok_h, tok, load_sem.at[3])
    own_down.start()
    own_up.start()
    load_gain = pltpu.make_async_copy(gain_h, gain_ref, load_sem.at[4])
    load_heads = pltpu.make_async_copy(heads_h, heads_ref, load_sem.at[5])
    load_gain.start()
    load_heads.start()
    load_cot.start()
    load_tok.start()

    barrier = pltpu.get_barrier_semaphore()
    others = [{"dp": after}, {"dp": before}, {"dp": sibling}, {"groups": partner}]
    others += [{"mp": (me_x + i) % n_mp} for i in range(1, n_mp)]
    for where in others:
        pl.semaphore_signal(barrier, inc=1, device_id=where, device_id_type=MESH)
    pl.semaphore_wait(barrier, len(others))

    def send_own_down():
        for part in (part_a, part_b):
            for way in (0, 1):
                z_copy(0, way, z, part).start()
        c_copy(0, z, core).start()

    wide = cols // 3

    def send_own_up(j):
        part = jnp.where(j < 3, part_a, part_b)
        rows = pl.ds(pl.multiple_of((2 * z + core) * up_rows + part * rows3, rows3), rows3)
        ref = wu.at[rows, pl.ds(pl.multiple_of((j % 3) * wide, 128), wide)]
        for way in (0, 1):
            remote(
                ref, ref, z_send.at[1], z_recv.at[1, part, z], {"dp": (after, before)[way]}
            ).start()

    def ring_a(kind, s):
        lz, rz = left(s), right(s)
        z_copy(kind, 0, lz, part_a).wait_recv()
        z_copy(kind, 0, lz, part_a).start()
        y_copy(kind, lz, part_a).start()
        z_copy(kind, 1, rz, part_a).wait_recv()

        @pl.when(s < half - 1)
        def _():
            z_copy(kind, 1, rz, part_a).start()

        y_copy(kind, rz, part_a).start()

    def ring_b(kind, s):
        lz, rz = left(s), right(s)
        z_copy(kind, 0, lz, part_b).wait_recv()

        @pl.when(s < half - 1)
        def _():
            z_copy(kind, 0, lz, part_b).start()

        z_copy(kind, 1, rz, part_b).wait_recv()
        z_copy(kind, 1, rz, part_b).start()
        if kind == 1:
            c_part(lz, 0).start()
            c_part(rz, 0).start()

    def ring_step(kind, s, between):
        ring_a(kind, s)
        between()
        ring_b(kind, s)

    far = right(half)

    x_peers = [((me_x + i) % n_mp, (me_x + n_mp - i) % n_mp) for i in range(1, n_mp)]
    per_x = n_z // n_mp

    def w2_at(owner, j, bc):
        return wd2.at[owner, pl.ds(pl.multiple_of((2 * j + bc) * down_rows, down_rows), down_rows), :]

    def w2_copy(bz):
        to = bz // per_x
        j = bz - to * per_x
        return remote(block(0, bz, core), w2_at(me_x, j, core), w2_send.at[0], w2_recv.at[0], {"mp": to})

    def pass_on(bz):
        @pl.when(bz // per_x != me_x)
        def _():
            w2_copy(bz).start()

    def w2_rows(i, j, bc):
        return w2_at(x_peers[i][1], j, bc)

    def w2_share(i, j, bc):
        ref = w2_rows(i, j, bc)
        return remote(ref, ref, w2c_send.at[0], w2c_recv.at[0], {"dp": sibling})

    def share(kind, bz):
        y_copy(kind, bz, part_c).wait_recv()
        if kind == 0:
            c_copy(0, bz, core).start()
            pass_on(bz)
        else:
            c_part(bz, 1).start()

    def share_pair(kind, s):
        share(kind, left(s))
        share(kind, right(s))

    def wait_sibling(kind, bz):
        c_copy(kind, bz, 1 - core).wait_recv()

    n_lane_tiles = cols // 128
    cut = n_lane_tiles * 3 // 4 * 128

    def far_part(bz):
        return pl.ds(pl.multiple_of((2 * bz + core) * up_rows + part_c * rows3, rows3), rows3)

    def far_copy(way):
        bz = (left, right)[way](half - 1)
        ref = wu.at[far_part(bz), (slice(0, cut), slice(cut, cols))[way]]
        return remote(ref, ref, far_send.at[0], z_recv.at[1, part_c, bz], {"dp": (after, before)[way]})

    lane1 = lax.broadcasted_iota(jnp.int32, (1, 128), 1)

    own_down.wait()
    send_own_down()
    own_up.wait()
    send_own_up(0)
    pass_on(z)
    c_copy(1, z, core).start()
    def gain_copy(i):
        return remote(
            gain_all.at[me_x], gain_all.at[me_x], ga_send.at[0], ga_recv.at[0], {"mp": x_peers[i][0]}
        )

    load_gain.wait()
    load_heads.wait()
    held = jnp.int32(0)
    for i in range(n_mp):
        held = held + jnp.where(me_x == i, heads_ref[i], 0)
    kept = held * HD
    gain_all[me_x] = gain_ref[...].reshape(1, lat_cols)
    load_cot.wait()
    n_blocks = cols // 128
    per_step = -(-n_blocks // (half - 1))

    def turn(j, _):
        at = pl.ds(pl.multiple_of(j * 128, 128), 128)
        value = jnp.where(lane1 + j * 128 < kept, cot[:, at], jnp.zeros((), BF16))
        cot_t[at, :] = value.T
        return 0

    def down_step(s, _):
        def between():
            @pl.when(s > 2)
            def _():
                share_pair(0, s - 2)

        ring_step(0, s, between)

        @pl.when(s <= 5)
        def _():
            send_own_up(s)

        @pl.when(s == 4)
        def _():
            z_copy(1, 0, left(1), part_a).wait_recv()
            y_copy(1, left(1), part_a).start()

        @pl.when(s == 5)
        def _():
            z_copy(1, 1, right(1), part_a).wait_recv()
            y_copy(1, right(1), part_a).start()

        @pl.when(s == 6)
        def _():
            z_copy(1, 0, left(1), part_a).start()
            z_copy(1, 1, right(1), part_a).start()

        lax.fori_loop((s - 1) * per_step, jnp.minimum(s * per_step, n_blocks), turn, 0)
        return 0

    lax.fori_loop(1, half, down_step, 0)
    z_copy(1, 0, left(1), part_b).wait_recv()
    z_copy(1, 0, left(1), part_b).start()
    z_copy(1, 1, right(1), part_b).wait_recv()
    z_copy(1, 1, right(1), part_b).start()
    c_part(left(1), 0).start()
    c_part(right(1), 0).start()
    for i in range(n_mp - 1):
        gain_copy(i).start()
    z_copy(0, 0, far, part_a).wait_recv()
    y_copy(0, far, part_a).start()
    z_copy(0, 1, far, part_b).wait_recv()
    ring_a(1, 2)
    share_pair(0, half - 2)
    share_pair(0, half - 1)
    share(0, far)
    ring_b(1, 2)
    load_tok.wait()

    from_sibling = wd.at[pl.ds(0, n_z * down_rows), :]
    remote(from_sibling, from_sibling, c_send.at[0], c_recv.at[n_z], {"dp": sibling}).wait_recv()

    k_size = width // 7

    def latent_part(k, total):
        at = pl.ds(pl.multiple_of(k * k_size, k_size), k_size)
        return total + jnp.dot(tok[:, at], wd[at, :], preferred_element_type=F32)

    latent_raw = lax.fori_loop(0, 7, latent_part, jnp.zeros((n_tok, lat_cols), F32))

    def lat_rows(owner):
        return pl.ds(pl.multiple_of(owner * lat_cols, lat_cols), lat_cols)

    lr_t[lat_rows(me_x), :] = latent_raw.T

    def lr_copy(i, owner):
        ref = lr_t.at[lat_rows(owner), :]
        return remote(ref, ref, lr_send.at[0], lr_recv.at[0], {"mp": x_peers[i][0]})

    for i in range(n_mp - 1):
        lr_copy(i, me_x).start()
    z_rows = 2 * up_rows

    def rows_of(bz):
        return pl.ds(pl.multiple_of(bz * z_rows, z_rows), z_rows)

    def gl_copy(i, bz):
        return remote(
            send_gl.at[rows_of(bz), :], peer_gl.at[i, rows_of(bz), :],
            gl_send.at[0], gl_recv.at[0], {"mp": x_peers[i][0]},
        )

    def publish(bz, value):
        own_gl[rows_of(bz), :] = value
        send_gl[rows_of(bz), :] = value.astype(BF16)

    def send_blocks(zs):
        for bz in zs:
            for i in range(n_mp - 1):
                gl_copy(i, bz).start()

    tiles = [(off, min(256, wide - off)) for off in range(0, wide, 256)]

    def compute(zs, gl=True, q=True, first=False, final=False):
        if q:
            one = jnp.concatenate([lat_t[rows_of(bz), :] for bz in zs], axis=0).T

        def step(c, total):
            for off, size in tiles:
                at = pl.ds(pl.multiple_of(c * wide + off, 128), size)
                tile = jnp.concatenate([wu[rows_of(bz), at] for bz in zs], axis=0)
                if gl:
                    total = total + jnp.dot(tile, cot_t[at, :], preferred_element_type=F32)
                if q:
                    value = jnp.dot(one, tile, preferred_element_type=F32)
                    if not first:
                        value = value + q_acc[:, at]
                    if final:
                        lane = lax.broadcasted_iota(jnp.int32, (1, size), 1) + (c * wide + off)
                        q_out[:, at] = jnp.where(lane < kept, value, 0.0).astype(BF16)
                    else:
                        q_acc[:, at] = value
            return total

        start = jnp.zeros((z_rows * len(zs), n_tok), F32) if gl else 0
        total = lax.fori_loop(0, 3, step, start)
        if gl:
            for k, bz in enumerate(zs):
                publish(bz, total[k * z_rows : (k + 1) * z_rows])
            send_blocks(zs)

    def pair(s):
        return [left(s), right(s)]

    def gl_pair(s):
        for bz in pair(s):
            wait_sibling(1, bz)
        compute(pair(s), q=False)

    def q_pair(s):
        compute(pair(s), gl=False)

    ring_a(1, 3)
    share_pair(1, 1)
    share_pair(1, 2)
    wait_sibling(1, z)
    compute([z], q=False)
    ring_b(1, 3)
    gl_pair(1)
    r_size = out_cols // 7

    def own_part(k, _):
        to = pl.ds(pl.multiple_of(k * r_size, r_size), r_size)
        came = pl.ds(pl.multiple_of(me_x * out_cols + k * r_size, r_size), r_size)
        wd2[me_x, to, :] = wd[came, :]
        return 0

    lax.fori_loop(0, 7, own_part, 0)
    ring_a(1, 4)
    share_pair(1, 3)
    gl_pair(2)
    ring_b(1, 4)

    def whole(ref, send, recv):
        return remote(ref, ref, send.at[0], recv.at[0], {"dp": sibling})

    w2_bytes = wd.at[pl.ds(0, (n_mp - 1) * per_x * down_rows), :]

    def w2_pass(j, _):
        for i in range(n_mp - 1):
            w2_share(i, j, core).start()
        return 0

    def middle(s, _):
        gl_pair(s - 2)
        ring_step(1, s, lambda: share_pair(1, s - 1))
        return 0

    lax.fori_loop(5, 7, middle, 0)
    gl_pair(5)
    gain_bytes = gain_all.at[pl.ds(0, n_mp - 1)]
    lat_bytes = lr_t.at[pl.ds(0, (n_mp - 1) * lat_cols), :]
    whole(gain_bytes, ga_send, ga_recv).wait_recv()
    for b in range(n_mp):
        gain_b[b * lat_cols : (b + 1) * lat_cols, :] = jnp.broadcast_to(gain_all[b], (n_tok, lat_cols)).T
    whole(lat_bytes, lr_send, lr_recv).wait_recv()
    squares = jnp.zeros((1, n_tok), F32)
    for b in range(n_mp):
        value = lr_t[b * lat_cols : (b + 1) * lat_cols, :]
        squares = squares + jnp.sum(value * value, axis=0, keepdims=True)
    root[...] = jnp.sqrt(squares / lat + 1e-06)
    for b in range(n_mp):
        at = slice(b * lat_cols, (b + 1) * lat_cols)
        lat_t[at, :] = (lr_t[at, :] / root[...] * gain_b[at, :]).astype(BF16)

    compute([z], gl=False, first=True)
    q_pair(1)
    ring_a(1, 7)
    share_pair(1, 6)
    q_pair(2)
    q_pair(3)
    ring_b(1, 7)
    gl_pair(6)
    q_pair(4)
    whole(w2_bytes, w2_send, w2_recv).wait_recv()
    lax.fori_loop(0, per_x, w2_pass, 0)
    for way in (0, 1):
        bz = (left, right)[way](half - 1)
        y_copy(1, bz, part_c).wait_recv()
        far_copy(way).start()
        c_part(bz, 1).start()
    z_copy(1, 0, far, part_a).wait_recv()
    z_copy(1, 1, far, part_b).wait_recv()
    c_part(far, 0).start()
    q_pair(5)
    z_copy(1, 0, far, part_c).wait_recv()
    c_part(far, 1).start()
    gl_pair(half - 1)
    wait_sibling(1, far)
    compute([far], q=False)
    q_pair(6)
    q_pair(7)
    compute([far], gl=False, final=True)
    q_store = pltpu.make_async_copy(q_out, q_h, out_sem.at[0])
    q_store.start()

    thirds = 2 * (n_z - 1)
    sends = [
        (wd.at[pl.ds(0, thirds * down_rows // 3), :], z_send.at[0]),
        (wu.at[pl.ds(0, thirds * rows3), :], z_send.at[1]),
        (wd.at[pl.ds(0, (n_z - 1) * down_rows // 3), :], y_send.at[0]),
        (wu.at[pl.ds(0, (n_z - 2) * rows3), :], y_send.at[1]),
        (wd.at[pl.ds(0, n_z * down_rows), :], c_send.at[0]),
        (wu.at[pl.ds(0, n_z * up_rows), :], c_send.at[1]),
        (wu.at[pl.ds(0, rows3), :], far_send.at[0]),
        (gain_bytes, ga_send.at[0]),
        (lat_bytes, lr_send.at[0]),
        (w2_bytes, w2_send.at[0]),
        (w2_bytes, w2c_send.at[0]),
        (peer_gl, gl_send.at[0]),
    ]
    for ref, sem in sends:
        remote(ref, ref, sem, c_recv.at[n_z], {"dp": sibling}).wait_send()
    whole(peer_gl, gl_send, gl_recv).wait_recv()
    inner = jnp.zeros((1, n_tok), F32)
    for b in range(n_mp):
        at = slice(b * lat_cols, (b + 1) * lat_cols)
        total = own_gl[at, :]
        for i in range(n_mp - 1):
            total = total + peer_gl[i, at, :].astype(F32)
        total = total * gain_b[at, :]
        own_gl[at, :] = total
        inner = inner + jnp.sum(total * lr_t[at, :], axis=0, keepdims=True)
    scale = inner / (lat * root[...] * root[...] * root[...])
    for b in range(n_mp):
        at = slice(b * lat_cols, (b + 1) * lat_cols)
        grad_raw[b] = (own_gl[at, :] / root[...] - lr_t[at, :] * scale).T.astype(BF16)
    whole(w2_bytes, w2c_send, w2c_recv).wait_recv()

    for k in range(7):
        at = slice(k * r_size, (k + 1) * r_size)
        total = jnp.zeros((n_tok, r_size), F32)
        for b in range(n_mp):
            total = total + lax.dot_general(
                grad_raw[b], wd2[b, at, :], (((1,), (1,)), ((), ())), preferred_element_type=F32
            )
        gt_out[:, at] = total.astype(BF16)
    gt_store = pltpu.make_async_copy(gt_out, gt_h, out_sem.at[1])
    gt_store.start()

    q_store.wait()
    gt_store.wait()


def write_kernel(q_in, gt_in, q_h, gt_h, q_hold, gt_hold, in_sem, out_sem):
    n_tok = q_in.shape[0]
    quarter = n_tok // 4
    pairs = [(q_in, q_hold, q_h, slice(k * quarter, (k + 1) * quarter)) for k in range(4)]
    pairs.append((gt_in, gt_hold, gt_h, slice(0, n_tok)))

    def load(k):
        src, hold, _, at = pairs[k]
        return pltpu.make_async_copy(src.at[at, :], hold.at[at, :], in_sem.at[k])

    def store(k):
        _, hold, dst, at = pairs[k]
        return pltpu.make_async_copy(hold.at[at, :], dst.at[at, :], out_sem.at[k])

    for k in range(len(pairs)):
        load(k).start()
    for k in range(len(pairs)):
        load(k).wait()
        store(k).start()
    for k in range(len(pairs)):
        store(k).wait()


def body(tokens, w_down, gain, w_up, head_counts, cotangent):
    n_dp, n_mp = lax.axis_size("dp"), lax.axis_size("mp")
    n_z = n_dp // 2
    n_tok, width = tokens.shape
    up_rows, cols = w_up.shape
    lat_cols = w_down.shape[1]
    lat = lat_cols * n_mp
    out_cols = width // n_mp
    dma = pltpu.SemaphoreType.DMA
    anywhere = pl.BlockSpec(memory_space=pl.ANY)
    peers = n_mp - 1
    queries, grad_tokens = pl.pallas_call(
        kernel,
        out_shape=(
            jax.ShapeDtypeStruct((n_tok, cols), BF16),
            jax.ShapeDtypeStruct((n_tok, out_cols), BF16),
        ),
        in_specs=[
            anywhere,
            anywhere,
            anywhere,
            anywhere,
            anywhere,
            anywhere,
        ],
        out_specs=(anywhere, anywhere),
        scratch_shapes=[
            pltpu.VMEM((n_tok, width), BF16),
            pltpu.VMEM((width, lat_cols), BF16),
            pltpu.VMEM((n_mp, out_cols, lat_cols), BF16),
            pltpu.VMEM((lat, cols), BF16),
            pltpu.VMEM((n_tok, cols), BF16),
            pltpu.VMEM((cols, n_tok), BF16),
            pltpu.VMEM((lat, n_tok), F32),
            pltpu.VMEM((lat, n_tok), BF16),
            pltpu.VMEM((lat, n_tok), F32),
            pltpu.VMEM((n_mp, 1, lat_cols), F32),
            pltpu.VMEM((lat, n_tok), F32),
            pltpu.VMEM((lat, n_tok), BF16),
            pltpu.VMEM((peers, lat, n_tok), BF16),
            pltpu.VMEM((n_mp, n_tok, lat_cols), BF16),
            pltpu.VMEM((n_tok, cols), F32),
            pltpu.VMEM((n_tok, cols), BF16),
            pltpu.VMEM((n_tok, out_cols), BF16),
            pltpu.VMEM((1, n_tok), F32),
            dma((6,)),
            dma((2,)),
            dma((2,)),
            dma((2, 3, n_z)),
            dma((2,)),
            dma((2,)),
            dma((n_z + 1,)),
            dma((1,)),
            dma((1,)),
            dma((1,)),
            dma((1,)),
            dma((1,)),
            dma((1,)),
            dma((1,)),
            dma((1,)),
            dma((1,)),
            dma((1,)),
            dma((1,)),
            pltpu.VMEM(gain.shape, F32),
            pltpu.SMEM(head_counts.shape, jnp.int32),
        ],
        compiler_params=pltpu.CompilerParams(
            collective_id=0, has_side_effects=True, vmem_limit_bytes=60 * 1024 * 1024
        ),
        name="gather_and_project",
    )(tokens, w_down, gain, w_up, head_counts, cotangent)
    return pl.pallas_call(
        write_kernel,
        out_shape=(
            jax.ShapeDtypeStruct((n_tok, cols), BF16),
            jax.ShapeDtypeStruct((n_tok, out_cols), BF16),
        ),
        in_specs=[anywhere, anywhere],
        out_specs=(anywhere, anywhere),
        scratch_shapes=[
            pltpu.VMEM((n_tok, cols), BF16),
            pltpu.VMEM((n_tok, out_cols), BF16),
            dma((5,)),
            dma((5,)),
        ],
        name="write_outputs",
    )(queries, grad_tokens)


def solution(mesh):
    in_specs = (
        P(("groups", "dp"), None),
        P("dp", "mp"),
        P("mp"),
        P("dp", "mp"),
        P(),
        P(("groups", "dp"), "mp"),
    )
    out_specs = (P(("groups", "dp"), "mp"), P(("groups", "dp"), "mp"))
    return jax.shard_map(body, mesh=mesh, in_specs=in_specs, out_specs=out_specs, check_vma=False)
```

```python
import functools

import jax
import jax.numpy as jnp
from jax import lax
from jax.experimental import pallas as pl
from jax.experimental.pallas import tpu as pltpu
from jax.sharding import PartitionSpec as P

HD = 192
MESH = pl.DeviceIdType.MESH
F32 = jnp.float32
BF16 = jnp.bfloat16


def kernel(
    tok_h, wd_h, gain_h, wu_h, heads_h, cot_h, q_h, gt_h,
    tok, wd, wd2, wu, cot, cot_t, lr_t, lat_t, gain_b, gain_all,
    own_gl, send_gl, peer_gl, grad_raw, q_acc, q_out, gt_out, root,
    load_sem, out_sem, z_send, z_recv, y_send, c_send, c_recv,
    lr_send, lr_recv, ga_send, ga_recv, w2_send, w2_recv, w2c_send, w2c_recv, gl_send, gl_recv,
    far_send, gain_ref, heads_ref,
):
    n_dp, n_mp = lax.axis_size("dp"), lax.axis_size("mp")
    n_z = n_dp // 2
    half = n_z // 2
    me_g, me_dp, me_x = lax.axis_index("groups"), lax.axis_index("dp"), lax.axis_index("mp")
    z, core = me_dp // 2, me_dp % 2
    plane = me_g % 2
    partner = me_g + 1 - 2 * plane
    after, before = (me_dp + 2) % n_dp, (me_dp + n_dp - 2) % n_dp
    sibling = me_dp + 1 - 2 * core

    up_rows, cols = wu_h.shape
    down_rows, lat_cols = wd_h.shape
    n_tok, width = tok_h.shape
    lat = lat_cols * n_mp
    out_cols = width // n_mp
    rows3, cols3 = up_rows // 3, lat_cols // 3
    part_a, part_b, part_c = 2 * plane, 1, 2 * (1 - plane)

    def block(kind, bz, bc):
        if kind == 0:
            return wd.at[pl.ds(pl.multiple_of((2 * bz + bc) * down_rows, down_rows), down_rows), :]
        return wu.at[pl.ds(pl.multiple_of((2 * bz + bc) * up_rows, up_rows), up_rows), :]

    def piece(kind, bz, part):
        if kind == 0:
            rows = pl.ds(pl.multiple_of((2 * bz + core) * down_rows, down_rows), down_rows)
            return wd.at[rows, pl.ds(pl.multiple_of(part * cols3, cols3), cols3)]
        return wu.at[pl.ds(pl.multiple_of((2 * bz + core) * up_rows + part * rows3, rows3), rows3), :]

    def remote(src, dst, send, recv, where):
        return pltpu.make_async_remote_copy(
            src_ref=src, dst_ref=dst, send_sem=send, recv_sem=recv, device_id=where, device_id_type=MESH
        )

    def z_copy(kind, way, bz, part):
        ref = piece(kind, bz, part)
        return remote(
            ref, ref, z_send.at[kind], z_recv.at[kind, part, bz], {"dp": (after, before)[way]}
        )

    def y_copy(kind, bz, part):
        ref = piece(kind, bz, part)
        return remote(ref, ref, y_send.at[kind], z_recv.at[kind, part, bz], {"groups": partner})

    def c_copy(kind, bz, bc):
        ref = block(kind, bz, bc)
        return remote(ref, ref, c_send.at[kind], c_recv.at[bz if kind else n_z], {"dp": sibling})

    def c_part(bz, which):
        base = (2 * bz + core) * up_rows
        if which == 0:
            rows = pl.ds(pl.multiple_of(base + plane * rows3, rows3), 2 * rows3)
        else:
            rows = pl.ds(pl.multiple_of(base + part_c * rows3, rows3), rows3)
        ref = wu.at[rows, :]
        return remote(ref, ref, c_send.at[1], c_recv.at[bz], {"dp": sibling})

    def left(s):
        return (z + n_z - s) % n_z

    def right(s):
        return (z + s) % n_z

    own_down = pltpu.make_async_copy(wd_h, block(0, z, core), load_sem.at[0])
    own_up = pltpu.make_async_copy(wu_h, block(1, z, core), load_sem.at[1])
    load_cot = pltpu.make_async_copy(cot_h, cot, load_sem.at[2])
    load_tok = pltpu.make_async_copy(tok_h, tok, load_sem.at[3])
    own_down.start()
    own_up.start()
    load_gain = pltpu.make_async_copy(gain_h, gain_ref, load_sem.at[4])
    load_heads = pltpu.make_async_copy(heads_h, heads_ref, load_sem.at[5])
    load_gain.start()
    load_heads.start()
    load_cot.start()
    load_tok.start()

    barrier = pltpu.get_barrier_semaphore()
    others = [{"dp": after}, {"dp": before}, {"dp": sibling}, {"groups": partner}]
    others += [{"mp": (me_x + i) % n_mp} for i in range(1, n_mp)]
    for where in others:
        pl.semaphore_signal(barrier, inc=1, device_id=where, device_id_type=MESH)
    pl.semaphore_wait(barrier, len(others))

    def send_own_down():
        for part in (part_a, part_b):
            for way in (0, 1):
                z_copy(0, way, z, part).start()
        c_copy(0, z, core).start()

    wide = cols // 3

    def send_own_up(j):
        part = jnp.where(j < 3, part_a, part_b)
        rows = pl.ds(pl.multiple_of((2 * z + core) * up_rows + part * rows3, rows3), rows3)
        ref = wu.at[rows, pl.ds(pl.multiple_of((j % 3) * wide, 128), wide)]
        for way in (0, 1):
            remote(
                ref, ref, z_send.at[1], z_recv.at[1, part, z], {"dp": (after, before)[way]}
            ).start()

    def ring_a(kind, s):
        lz, rz = left(s), right(s)
        z_copy(kind, 0, lz, part_a).wait_recv()
        z_copy(kind, 0, lz, part_a).start()
        y_copy(kind, lz, part_a).start()
        z_copy(kind, 1, rz, part_a).wait_recv()

        @pl.when(s < half - 1)
        def _():
            z_copy(kind, 1, rz, part_a).start()

        y_copy(kind, rz, part_a).start()

    def ring_b(kind, s):
        lz, rz = left(s), right(s)
        z_copy(kind, 0, lz, part_b).wait_recv()

        @pl.when(s < half - 1)
        def _():
            z_copy(kind, 0, lz, part_b).start()

        z_copy(kind, 1, rz, part_b).wait_recv()
        z_copy(kind, 1, rz, part_b).start()
        if kind == 1:
            c_part(lz, 0).start()
            c_part(rz, 0).start()

    def ring_step(kind, s, between):
        ring_a(kind, s)
        between()
        ring_b(kind, s)

    far = right(half)

    x_peers = [((me_x + i) % n_mp, (me_x + n_mp - i) % n_mp) for i in range(1, n_mp)]
    per_x = n_z // n_mp

    def w2_at(owner, j, bc):
        return wd2.at[owner, pl.ds(pl.multiple_of((2 * j + bc) * down_rows, down_rows), down_rows), :]

    def w2_copy(bz):
        to = bz // per_x
        j = bz - to * per_x
        return remote(block(0, bz, core), w2_at(me_x, j, core), w2_send.at[0], w2_recv.at[0], {"mp": to})

    def pass_on(bz):
        @pl.when(bz // per_x != me_x)
        def _():
            w2_copy(bz).start()

    def w2_rows(i, j, bc):
        return w2_at(x_peers[i][1], j, bc)

    def w2_share(i, j, bc):
        ref = w2_rows(i, j, bc)
        return remote(ref, ref, w2c_send.at[0], w2c_recv.at[0], {"dp": sibling})

    def share(kind, bz):
        y_copy(kind, bz, part_c).wait_recv()
        if kind == 0:
            c_copy(0, bz, core).start()
            pass_on(bz)
        else:
            c_part(bz, 1).start()

    def share_pair(kind, s):
        share(kind, left(s))
        share(kind, right(s))

    def wait_sibling(kind, bz):
        c_copy(kind, bz, 1 - core).wait_recv()

    n_lane_tiles = cols // 128
    cut = n_lane_tiles * 3 // 4 * 128

    def far_part(bz):
        return pl.ds(pl.multiple_of((2 * bz + core) * up_rows + part_c * rows3, rows3), rows3)

    def far_copy(way):
        bz = (left, right)[way](half - 1)
        ref = wu.at[far_part(bz), (slice(0, cut), slice(cut, cols))[way]]
        return remote(ref, ref, far_send.at[0], z_recv.at[1, part_c, bz], {"dp": (after, before)[way]})

    lane1 = lax.broadcasted_iota(jnp.int32, (1, 128), 1)

    own_down.wait()
    send_own_down()
    own_up.wait()
    send_own_up(0)
    pass_on(z)
    c_copy(1, z, core).start()
    def gain_copy(i):
        return remote(
            gain_all.at[me_x], gain_all.at[me_x], ga_send.at[0], ga_recv.at[0], {"mp": x_peers[i][0]}
        )

    load_gain.wait()
    load_heads.wait()
    held = jnp.int32(0)
    for i in range(n_mp):
        held = held + jnp.where(me_x == i, heads_ref[i], 0)
    kept = held * HD
    gain_all[me_x] = gain_ref[...].reshape(1, lat_cols)
    load_cot.wait()
    n_blocks = cols // 128
    per_step = -(-n_blocks // (half - 1))

    def turn(j, _):
        at = pl.ds(pl.multiple_of(j * 128, 128), 128)
        value = jnp.where(lane1 + j * 128 < kept, cot[:, at], jnp.zeros((), BF16))
        cot_t[at, :] = value.T
        return 0

    def down_step(s, _):
        def between():
            @pl.when(s > 2)
            def _():
                share_pair(0, s - 2)

        ring_step(0, s, between)

        @pl.when(s <= 5)
        def _():
            send_own_up(s)

        @pl.when(s == 4)
        def _():
            z_copy(1, 0, left(1), part_a).wait_recv()
            y_copy(1, left(1), part_a).start()

        @pl.when(s == 5)
        def _():
            z_copy(1, 1, right(1), part_a).wait_recv()
            y_copy(1, right(1), part_a).start()

        @pl.when(s == 6)
        def _():
            z_copy(1, 0, left(1), part_a).start()
            z_copy(1, 1, right(1), part_a).start()

        lax.fori_loop((s - 1) * per_step, jnp.minimum(s * per_step, n_blocks), turn, 0)
        return 0

    lax.fori_loop(1, half, down_step, 0)
    z_copy(1, 0, left(1), part_b).wait_recv()
    z_copy(1, 0, left(1), part_b).start()
    z_copy(1, 1, right(1), part_b).wait_recv()
    z_copy(1, 1, right(1), part_b).start()
    c_part(left(1), 0).start()
    c_part(right(1), 0).start()
    for i in range(n_mp - 1):
        gain_copy(i).start()
    z_copy(0, 0, far, part_a).wait_recv()
    y_copy(0, far, part_a).start()
    z_copy(0, 1, far, part_b).wait_recv()
    ring_a(1, 2)
    share_pair(0, half - 2)
    share_pair(0, half - 1)
    share(0, far)
    ring_b(1, 2)
    load_tok.wait()

    from_sibling = wd.at[pl.ds(0, n_z * down_rows), :]
    remote(from_sibling, from_sibling, c_send.at[0], c_recv.at[n_z], {"dp": sibling}).wait_recv()

    k_size = width // 7

    def latent_part(k, total):
        at = pl.ds(pl.multiple_of(k * k_size, k_size), k_size)
        return total + jnp.dot(tok[:, at], wd[at, :], preferred_element_type=F32)

    latent_raw = lax.fori_loop(0, 7, latent_part, jnp.zeros((n_tok, lat_cols), F32))

    def lat_rows(owner):
        return pl.ds(pl.multiple_of(owner * lat_cols, lat_cols), lat_cols)

    lr_t[lat_rows(me_x), :] = latent_raw.T

    def lr_copy(i, owner):
        ref = lr_t.at[lat_rows(owner), :]
        return remote(ref, ref, lr_send.at[0], lr_recv.at[0], {"mp": x_peers[i][0]})

    for i in range(n_mp - 1):
        lr_copy(i, me_x).start()
    z_rows = 2 * up_rows

    def rows_of(bz):
        return pl.ds(pl.multiple_of(bz * z_rows, z_rows), z_rows)

    def gl_copy(i, bz):
        return remote(
            send_gl.at[rows_of(bz), :], peer_gl.at[i, rows_of(bz), :],
            gl_send.at[0], gl_recv.at[0], {"mp": x_peers[i][0]},
        )

    def publish(bz, value):
        own_gl[rows_of(bz), :] = value
        send_gl[rows_of(bz), :] = value.astype(BF16)

    def send_blocks(zs):
        for bz in zs:
            for i in range(n_mp - 1):
                gl_copy(i, bz).start()

    tiles = [(off, min(256, wide - off)) for off in range(0, wide, 256)]

    def compute(zs, gl=True, q=True, first=False, final=False):
        if q:
            one = jnp.concatenate([lat_t[rows_of(bz), :] for bz in zs], axis=0).T

        def step(c, total):
            for off, size in tiles:
                at = pl.ds(pl.multiple_of(c * wide + off, 128), size)
                tile = jnp.concatenate([wu[rows_of(bz), at] for bz in zs], axis=0)
                if gl:
                    total = total + jnp.dot(tile, cot_t[at, :], preferred_element_type=F32)
                if q:
                    value = jnp.dot(one, tile, preferred_element_type=F32)
                    if not first:
                        value = value + q_acc[:, at]
                    if final:
                        lane = lax.broadcasted_iota(jnp.int32, (1, size), 1) + (c * wide + off)
                        q_out[:, at] = jnp.where(lane < kept, value, 0.0).astype(BF16)
                    else:
                        q_acc[:, at] = value
            return total

        start = jnp.zeros((z_rows * len(zs), n_tok), F32) if gl else 0
        total = lax.fori_loop(0, 3, step, start)
        if gl:
            for k, bz in enumerate(zs):
                publish(bz, total[k * z_rows : (k + 1) * z_rows])
            send_blocks(zs)

    def pair(s):
        return [left(s), right(s)]

    def gl_pair(s):
        for bz in pair(s):
            wait_sibling(1, bz)
        compute(pair(s), q=False)

    def q_pair(s):
        compute(pair(s), gl=False)

    ring_a(1, 3)
    share_pair(1, 1)
    share_pair(1, 2)
    wait_sibling(1, z)
    compute([z], q=False)
    ring_b(1, 3)
    gl_pair(1)
    r_size = out_cols // 7

    def own_part(k, _):
        to = pl.ds(pl.multiple_of(k * r_size, r_size), r_size)
        came = pl.ds(pl.multiple_of(me_x * out_cols + k * r_size, r_size), r_size)
        wd2[me_x, to, :] = wd[came, :]
        return 0

    lax.fori_loop(0, 7, own_part, 0)
    ring_a(1, 4)
    share_pair(1, 3)
    gl_pair(2)
    ring_b(1, 4)

    def whole(ref, send, recv):
        return remote(ref, ref, send.at[0], recv.at[0], {"dp": sibling})

    w2_bytes = wd.at[pl.ds(0, (n_mp - 1) * per_x * down_rows), :]

    def w2_pass(j, _):
        for i in range(n_mp - 1):
            w2_share(i, j, core).start()
        return 0

    def middle(s, _):
        gl_pair(s - 2)
        ring_step(1, s, lambda: share_pair(1, s - 1))
        return 0

    lax.fori_loop(5, 7, middle, 0)
    gl_pair(5)
    gain_bytes = gain_all.at[pl.ds(0, n_mp - 1)]
    lat_bytes = lr_t.at[pl.ds(0, (n_mp - 1) * lat_cols), :]
    whole(gain_bytes, ga_send, ga_recv).wait_recv()
    for b in range(n_mp):
        gain_b[b * lat_cols : (b + 1) * lat_cols, :] = jnp.broadcast_to(gain_all[b], (n_tok, lat_cols)).T
    whole(lat_bytes, lr_send, lr_recv).wait_recv()
    squares = jnp.zeros((1, n_tok), F32)
    for b in range(n_mp):
        value = lr_t[b * lat_cols : (b + 1) * lat_cols, :]
        squares = squares + jnp.sum(value * value, axis=0, keepdims=True)
    root[...] = jnp.sqrt(squares / lat + 1e-06)
    for b in range(n_mp):
        at = slice(b * lat_cols, (b + 1) * lat_cols)
        lat_t[at, :] = (lr_t[at, :] / root[...] * gain_b[at, :]).astype(BF16)

    compute([z], gl=False, first=True)
    q_pair(1)
    ring_a(1, 7)
    share_pair(1, 6)
    q_pair(2)
    q_pair(3)
    ring_b(1, 7)
    gl_pair(6)
    q_pair(4)
    whole(w2_bytes, w2_send, w2_recv).wait_recv()
    lax.fori_loop(0, per_x, w2_pass, 0)
    for way in (0, 1):
        bz = (left, right)[way](half - 1)
        y_copy(1, bz, part_c).wait_recv()
        far_copy(way).start()
        c_part(bz, 1).start()
    z_copy(1, 0, far, part_a).wait_recv()
    z_copy(1, 1, far, part_b).wait_recv()
    c_part(far, 0).start()
    q_pair(5)
    z_copy(1, 0, far, part_c).wait_recv()
    c_part(far, 1).start()
    gl_pair(half - 1)
    wait_sibling(1, far)
    compute([far], q=False)
    q_pair(6)
    q_pair(7)
    compute([far], gl=False, final=True)
    q_store = pltpu.make_async_copy(q_out, q_h, out_sem.at[0])
    q_store.start()

    thirds = 2 * (n_z - 1)
    sends = [
        (wd.at[pl.ds(0, thirds * down_rows // 3), :], z_send.at[0]),
        (wu.at[pl.ds(0, thirds * rows3), :], z_send.at[1]),
        (wd.at[pl.ds(0, (n_z - 1) * down_rows // 3), :], y_send.at[0]),
        (wu.at[pl.ds(0, (n_z - 2) * rows3), :], y_send.at[1]),
        (wd.at[pl.ds(0, n_z * down_rows), :], c_send.at[0]),
        (wu.at[pl.ds(0, n_z * up_rows), :], c_send.at[1]),
        (wu.at[pl.ds(0, rows3), :], far_send.at[0]),
        (gain_bytes, ga_send.at[0]),
        (lat_bytes, lr_send.at[0]),
        (w2_bytes, w2_send.at[0]),
        (w2_bytes, w2c_send.at[0]),
        (peer_gl, gl_send.at[0]),
    ]
    for ref, sem in sends:
        remote(ref, ref, sem, c_recv.at[n_z], {"dp": sibling}).wait_send()
    whole(peer_gl, gl_send, gl_recv).wait_recv()
    inner = jnp.zeros((1, n_tok), F32)
    for b in range(n_mp):
        at = slice(b * lat_cols, (b + 1) * lat_cols)
        total = own_gl[at, :]
        for i in range(n_mp - 1):
            total = total + peer_gl[i, at, :].astype(F32)
        total = total * gain_b[at, :]
        own_gl[at, :] = total
        inner = inner + jnp.sum(total * lr_t[at, :], axis=0, keepdims=True)
    scale = inner / (lat * root[...] * root[...] * root[...])
    for b in range(n_mp):
        at = slice(b * lat_cols, (b + 1) * lat_cols)
        grad_raw[b] = (own_gl[at, :] / root[...] - lr_t[at, :] * scale).T.astype(BF16)
    whole(w2_bytes, w2c_send, w2c_recv).wait_recv()

    split = 4 * r_size

    def gt_store(k):
        at = (slice(0, split), slice(split, out_cols))[k]
        return pltpu.make_async_copy(gt_out.at[:, at], gt_h.at[:, at], out_sem.at[1 + k])

    for k in range(7):
        at = slice(k * r_size, (k + 1) * r_size)
        total = jnp.zeros((n_tok, r_size), F32)
        for b in range(n_mp):
            total = total + lax.dot_general(
                grad_raw[b], wd2[b, at, :], (((1,), (1,)), ((), ())), preferred_element_type=F32
            )
        gt_out[:, at] = total.astype(BF16)
        if k == 3:
            gt_store(0).start()
    gt_store(1).start()

    q_store.wait()
    gt_store(0).wait()
    gt_store(1).wait()


def write_kernel(q_in, gt_in, q_h, gt_h, q_hold, gt_hold, in_sem, out_sem):
    n_tok = q_in.shape[0]
    size = n_tok // 8
    pairs = [(q_in, q_hold, q_h, slice(k * size, (k + 1) * size)) for k in range(8)]
    pairs.append((gt_in, gt_hold, gt_h, slice(0, n_tok)))

    def load(k):
        src, hold, _, at = pairs[k]
        return pltpu.make_async_copy(src.at[at, :], hold.at[at, :], in_sem.at[k])

    def store(k):
        _, hold, dst, at = pairs[k]
        return pltpu.make_async_copy(hold.at[at, :], dst.at[at, :], out_sem.at[k])

    for k in range(len(pairs)):
        load(k).start()
    for k in range(len(pairs)):
        load(k).wait()
        store(k).start()
    for k in range(len(pairs)):
        store(k).wait()


def body(tokens, w_down, gain, w_up, head_counts, cotangent):
    n_dp, n_mp = lax.axis_size("dp"), lax.axis_size("mp")
    n_z = n_dp // 2
    n_tok, width = tokens.shape
    up_rows, cols = w_up.shape
    lat_cols = w_down.shape[1]
    lat = lat_cols * n_mp
    out_cols = width // n_mp
    dma = pltpu.SemaphoreType.DMA
    anywhere = pl.BlockSpec(memory_space=pl.ANY)
    peers = n_mp - 1
    queries, grad_tokens = pl.pallas_call(
        kernel,
        out_shape=(
            jax.ShapeDtypeStruct((n_tok, cols), BF16),
            jax.ShapeDtypeStruct((n_tok, out_cols), BF16),
        ),
        in_specs=[
            anywhere,
            anywhere,
            anywhere,
            anywhere,
            anywhere,
            anywhere,
        ],
        out_specs=(anywhere, anywhere),
        scratch_shapes=[
            pltpu.VMEM((n_tok, width), BF16),
            pltpu.VMEM((width, lat_cols), BF16),
            pltpu.VMEM((n_mp, out_cols, lat_cols), BF16),
            pltpu.VMEM((lat, cols), BF16),
            pltpu.VMEM((n_tok, cols), BF16),
            pltpu.VMEM((cols, n_tok), BF16),
            pltpu.VMEM((lat, n_tok), F32),
            pltpu.VMEM((lat, n_tok), BF16),
            pltpu.VMEM((lat, n_tok), F32),
            pltpu.VMEM((n_mp, 1, lat_cols), F32),
            pltpu.VMEM((lat, n_tok), F32),
            pltpu.VMEM((lat, n_tok), BF16),
            pltpu.VMEM((peers, lat, n_tok), BF16),
            pltpu.VMEM((n_mp, n_tok, lat_cols), BF16),
            pltpu.VMEM((n_tok, cols), F32),
            pltpu.VMEM((n_tok, cols), BF16),
            pltpu.VMEM((n_tok, out_cols), BF16),
            pltpu.VMEM((1, n_tok), F32),
            dma((6,)),
            dma((3,)),
            dma((2,)),
            dma((2, 3, n_z)),
            dma((2,)),
            dma((2,)),
            dma((n_z + 1,)),
            dma((1,)),
            dma((1,)),
            dma((1,)),
            dma((1,)),
            dma((1,)),
            dma((1,)),
            dma((1,)),
            dma((1,)),
            dma((1,)),
            dma((1,)),
            dma((1,)),
            pltpu.VMEM(gain.shape, F32),
            pltpu.SMEM(head_counts.shape, jnp.int32),
        ],
        compiler_params=pltpu.CompilerParams(
            collective_id=0, has_side_effects=True, vmem_limit_bytes=60 * 1024 * 1024
        ),
        name="gather_and_project",
    )(tokens, w_down, gain, w_up, head_counts, cotangent)
    return pl.pallas_call(
        write_kernel,
        out_shape=(
            jax.ShapeDtypeStruct((n_tok, cols), BF16),
            jax.ShapeDtypeStruct((n_tok, out_cols), BF16),
        ),
        in_specs=[anywhere, anywhere],
        out_specs=(anywhere, anywhere),
        scratch_shapes=[
            pltpu.VMEM((n_tok, cols), BF16),
            pltpu.VMEM((n_tok, out_cols), BF16),
            dma((9,)),
            dma((9,)),
        ],
        name="write_outputs",
    )(queries, grad_tokens)


def solution(mesh):
    in_specs = (
        P(("groups", "dp"), None),
        P("dp", "mp"),
        P("mp"),
        P("dp", "mp"),
        P(),
        P(("groups", "dp"), "mp"),
    )
    out_specs = (P(("groups", "dp"), "mp"), P(("groups", "dp"), "mp"))
    return jax.shard_map(body, mesh=mesh, in_specs=in_specs, out_specs=out_specs, check_vma=False)
```
